256 devices in a mesh: gx: 4 (over y), gy: 8 (over x, core), gz: 8 (over z).
Axes of the slice: x: 4, y: 4, z: 8, core: 2. Of those that a mesh axis runs over, the one named last changes fastest.
Arguments:
- old_pos: float32 [3, 4, 8, 8, 1536], P(None, 'gx', 'gy', 'gz'), may hold values from -6 to 6
- displacement: float32 [3, 4, 8, 8, 1536], P(None, 'gx', 'gy', 'gz'), may hold values from -0.3 to 0.3
- inv_mass: float32 [4, 8, 8, 1536], P('gx', 'gy', 'gz'), may hold values from 0.0625 to 1
- bond_head: int32 [4, 8, 8, 1024], P('gx', 'gy', 'gz'), may hold values from 0 to 1535, as said below
- bond_tail: int32 [4, 8, 8, 1024], P('gx', 'gy', 'gz'), may hold values from 0 to 1967, as said below
- send_list: int32 [4, 8, 8, 16], P('gx', 'gy', 'gz'), may hold values from 0 to 1535, as said below
Outputs:
- new_pos: float32 [3, 4, 8, 8, 1536], P(None, 'gx', 'gy', 'gz')
- multipliers: float32 [4, 8, 8, 1024], P('gx', 'gy', 'gz')
The draws below stay inside these ranges and needn't reach their ends.
Inputs may be any that keep to these rules, and one draw needn't show every extreme that they name: `bond_head`: distinct atoms of the owning domain; no atom is the first atom of two constraints. `bond_tail`: below 1536: an atom of the owning domain other than the constraint's first atom, never in send_list; otherwise a slot 1536 + block * 16 + entry with block in 0..26 other than 13, distinct within a domain; 192 constraints of each domain use such slots. `send_list`: distinct atoms of the domain; a send atom is never a constraint's first atom and never a local second atom.
All inputs are finite; a program needn't handle non-finite values.
Results may differ from the reference program's by a relative error of at most 0.0011.
Values sent between devices are 32-bit elements; how exact they have to be, the bound alone decides.
A program may use at most 64 MiB of HBM per device.

```python
import math
import jax
import jax.numpy as jnp
from jax import lax

ATOM_DEV = 1536
CON_DEV = 1024
SEND = 16
HALO_CON = 192
ORDER = 4
DOM_X = 4
DOM_Y = 8
DOM_Z = 8


def layout(key):
    base = jax.random.fold_in(key, 7)
    keys = jax.random.split(base, DOM_X * DOM_Y * DOM_Z)

    def domain(dom_key):
        key_perm, key_pick, key_slot = jax.random.split(dom_key, 3)
        order = jax.random.permutation(key_perm, ATOM_DEV).astype(jnp.int32)
        sending = order[ATOM_DEV - SEND:]
        heads = order[:CON_DEV]
        local_tail = order[1:CON_DEV + 1]
        picked = jax.random.permutation(key_pick, CON_DEV).astype(jnp.int32)[:HALO_CON]
        slots = jax.random.permutation(key_slot, 26 * SEND).astype(jnp.int32)[:HALO_CON]
        block = slots // SEND
        block = block + (block >= 13).astype(jnp.int32)
        halo_tail = ATOM_DEV + block * SEND + slots % SEND
        tails = local_tail.at[picked].set(halo_tail.astype(jnp.int32))
        return (sending, heads, tails)
    sending, heads, tails = jax.vmap(domain)(keys)
    return (sending.reshape(DOM_X, DOM_Y, DOM_Z, SEND).astype(jnp.int32), heads.reshape(DOM_X, DOM_Y, DOM_Z, CON_DEV).astype(jnp.int32), tails.reshape(DOM_X, DOM_Y, DOM_Z, CON_DEV).astype(jnp.int32))


def draw_bond_head(key, part):
    return layout(key)[1]


def draw_bond_tail(key, part):
    return layout(key)[2]


def draw_send_list(key, part):
    return layout(key)[0]


def block_scale(own_key, shape, cuts, smallest, high):
    def one(position, shards_of):
        heights = jax.random.uniform(jax.random.fold_in(jax.random.fold_in(own_key, 6), position), (shards_of,), jnp.float32, smallest / len(cuts), high / len(cuts))
        return jnp.repeat(jnp.exp(heights), shape[position] // shards_of).reshape((-1,) + (1,) * (len(shape) - position - 1))

    factor_of = one(*cuts[0])
    for cut in cuts[1:]:
        factor_of = factor_of * one(*cut)
    return factor_of


def scatter_about(rng, extent, width, most, pieces=(), kind=jnp.bfloat16):
    array = jax.random.normal(rng, extent, jnp.float32) * width
    if len(pieces) > 0:
        array = block_scale(rng, extent, pieces, -0.22, 0.18) * array
    return jnp.clip(array, min=-most, max=most).astype(kind)


def setup_inputs(seed: int = 0) -> dict:
    splits = jax.random.split(jax.random.key(seed), 7)
    old_pos = scatter_about(splits[0], (3, DOM_X, DOM_Y, DOM_Z, ATOM_DEV), 1.0, 6.0, ((1, 4), (2, 8), (3, 8)), jnp.float32)
    displacement = scatter_about(splits[1], (3, DOM_X, DOM_Y, DOM_Z, ATOM_DEV), 0.05, 0.3, ((1, 4), (2, 8), (3, 8)), jnp.float32)
    inv_mass = jnp.clip(jnp.exp(math.log(1.0) - 2.7725887 * jax.random.uniform(splits[2], (DOM_X, DOM_Y, DOM_Z, ATOM_DEV), jnp.float32) ** block_scale(splits[2], (DOM_X, DOM_Y, DOM_Z, ATOM_DEV), ((0, 4), (1, 8), (2, 8)), -0.2, 0.2)), 0.0625, 1.0)
    bond_head = draw_bond_head(jax.random.fold_in(splits[6], 71), 0)
    bond_tail = draw_bond_tail(jax.random.fold_in(splits[6], 71), 0)
    send_list = draw_send_list(jax.random.fold_in(splits[6], 71), 0)
    return {"old_pos": old_pos, "displacement": displacement, "inv_mass": inv_mass, "bond_head": bond_head, "bond_tail": bond_tail, "send_list": send_list}


def global_index(bond_head, bond_tail, send_list):
    axis_x = jnp.arange(DOM_X, dtype=jnp.int32)[:, None, None, None]
    axis_y = jnp.arange(DOM_Y, dtype=jnp.int32)[None, :, None, None]
    axis_z = jnp.arange(DOM_Z, dtype=jnp.int32)[None, None, :, None]
    flat_dev = (axis_x * DOM_Y + axis_y) * DOM_Z + axis_z
    head = (flat_dev * ATOM_DEV + bond_head).reshape(-1)
    is_local = bond_tail < ATOM_DEV
    slot = jnp.maximum(bond_tail - ATOM_DEV, 0)
    block = slot // SEND
    entry = slot % SEND
    near_x = (axis_x + block // 9 - 1) % DOM_X
    near_y = (axis_y + block // 3 % 3 - 1) % DOM_Y
    near_z = (axis_z + block % 3 - 1) % DOM_Z
    neigh = (near_x * DOM_Y + near_y) * DOM_Z + near_z
    remote = send_list.reshape(-1)[(neigh * SEND + entry).reshape(-1)].reshape(neigh.shape)
    tail = jnp.where(is_local, flat_dev * ATOM_DEV + bond_tail, neigh * ATOM_DEV + remote)
    return (head.astype(jnp.int32), tail.reshape(-1).astype(jnp.int32))

def reference(old_pos, displacement, inv_mass, bond_head, bond_tail, send_list):
    head, tail = global_index(bond_head, bond_tail, send_list)
    old_flat = old_pos.reshape(3, -1)
    pos_now = old_flat + displacement.reshape(3, -1)
    masses = inv_mass.reshape(1, -1)
    total_atoms = old_flat.shape[1]
    bond_old = old_flat[:, head] - old_flat[:, tail]
    length = jnp.maximum(jnp.sqrt(lax.optimization_barrier(jnp.sum(bond_old * bond_old, axis=0))), 0.5)
    direction = bond_old / length
    bond_scale = 1.0 / jnp.sqrt(masses[0, head] + masses[0, tail])

    def spread(values):
        weighted = bond_scale * values * direction
        buffer = jnp.zeros((3, total_atoms), jnp.float32)
        buffer = buffer.at[:, head].add(weighted).at[:, tail].add(-weighted)
        return masses * buffer

    def couple(values):
        shift_vec = spread(values)
        return values - bond_scale * lax.optimization_barrier(jnp.sum(direction * (shift_vec[:, head] - shift_vec[:, tail]), axis=0))

    def expand(right_side):
        solution = right_side
        series = right_side
        for sweep in range(ORDER):
            series = couple(series)
            solution = solution + series
        return solution
    right_one = bond_scale * (lax.optimization_barrier(jnp.sum(direction * (pos_now[:, head] - pos_now[:, tail]), axis=0)) - length)
    sol_one = expand(right_one)
    pos_now = pos_now - spread(sol_one)
    stretch = pos_now[:, head] - pos_now[:, tail]
    current = lax.optimization_barrier(jnp.sum(stretch * stretch, axis=0))
    target = jnp.sqrt(jnp.maximum(2.0 * length * length - current, 0.5 * length * length))
    sol_two = expand(bond_scale * (length - target))
    pos_now = pos_now - spread(sol_two)
    return (pos_now.reshape(old_pos.shape), (sol_one + sol_two).reshape(bond_head.shape))
```

```python
import functools

import jax
import jax.numpy as jnp
from jax import lax
from jax.experimental import pallas as pl
from jax.experimental.pallas import tpu as pltpu
from jax.sharding import PartitionSpec as P

MESH = pl.DeviceIdType.MESH
ATOMS = 1536
BONDS = 1024
SEND = 16
LANES = 128
AT = ATOMS // LANES
BT = BONDS // LANES
ST = 4
BLOCKS = [b for b in range(27) if b != 13]
ROW_OF = {b: n for n, b in enumerate(BLOCKS)}
F32 = jnp.float32
I32 = jnp.int32
PAIRS = [(0, 0), (0, 1), (0, 2), (1, 1), (1, 2), (2, 2)]


def take(rows, lane):
    numbers = lax.GatherDimensionNumbers(
        offset_dims=(),
        collapsed_slice_dims=(1,),
        start_index_map=(1,),
        operand_batching_dims=(0,),
        start_indices_batching_dims=(0,),
    )
    return lax.gather(
        rows, lane[..., None], numbers, (1, 1), mode=lax.GatherScatterMode.PROMISE_IN_BOUNDS
    )


def lookup(tiles, tile, lane):
    out = jnp.zeros(lane.shape, F32)
    for j, row in enumerate(tiles):
        out = jnp.where(tile == j, take(jnp.broadcast_to(row, lane.shape), lane), out)
    return out


def kernel(
    sizes,
    old_ref,
    move_ref,
    mass_ref,
    head_ref,
    tail_ref,
    send_ref,
    new_ref,
    mult_ref,
    table,
    idx,
    cols,
    incidence,
    coupling,
    inverse,
    vec,
    rows,
    sums,
    kinds,
    gathered,
    r0_out,
    a_out,
    a2_out,
    b_out,
    c_out,
    d_out,
    r0_in,
    a_in,
    a2_in,
    b_in,
    c_in,
    d_in,
    send_sem,
    recv_sem,
):
    names = ("gx", "gy", "gz")
    me = [lax.axis_index(n) for n in names]

    def device(block, sign):
        offs = (block // 9 - 1, block // 3 % 3 - 1, block % 3 - 1)
        return tuple(lax.rem(m + sign * o + n, n) for m, o, n in zip(me, offs, sizes))

    barrier = pltpu.get_barrier_semaphore()
    for b in BLOCKS:
        pl.semaphore_signal(barrier, inc=1, device_id=device(b, 1), device_id_type=MESH)

    def start(stage, source, target, sign):
        for b in BLOCKS:
            pltpu.make_async_remote_copy(
                src_ref=source(b),
                dst_ref=target.at[ROW_OF[b]],
                send_sem=send_sem.at[stage],
                recv_sem=recv_sem.at[stage],
                device_id=device(b, sign),
                device_id_type=MESH,
            ).start()

    def all_of(stage, target):
        return pltpu.make_async_remote_copy(
            src_ref=target,
            dst_ref=target,
            send_sem=send_sem.at[stage],
            recv_sem=recv_sem.at[stage],
            device_id=device(0, 1),
            device_id_type=MESH,
        )

    lane8 = lax.broadcasted_iota(I32, (8, LANES), 1)
    group8 = lane8 // SEND
    sub128 = lax.broadcasted_iota(I32, (LANES, LANES), 0)
    lane128 = lax.broadcasted_iota(I32, (LANES, LANES), 1)
    eye = sub128 == lane128

    for j in range(AT):
        cut = pl.ds(j * LANES, LANES)
        for i in range(3):
            table[j, i : i + 1, :] = old_ref[i, :, cut]
            table[j, 3 + i : 4 + i, :] = move_ref[i, :, cut]
        table[j, 6:7, :] = mass_ref[:, cut]
        table[j, 7:8, :] = jnp.zeros((1, LANES), F32)
    sent8 = jnp.broadcast_to(
        jnp.concatenate([send_ref[...]] * (LANES // SEND), axis=1), (8, LANES)
    )
    mine = jnp.zeros((8, LANES), F32)
    for j in range(AT):
        mine = jnp.where(sent8 // LANES == j, take(table[j], sent8 % LANES), mine)
    r0_out[...] = mine
    pl.semaphore_wait(barrier, len(BLOCKS))
    start(0, lambda b: r0_out, r0_in, -1)

    for t in range(BT):
        cut = pl.ds(t * LANES, LANES)
        idx[0, t : t + 1, :] = head_ref[:, cut]
        idx[1, t : t + 1, :] = tail_ref[:, cut]
    head = idx[0]
    tail = idx[1]
    is_halo = tail >= ATOMS
    slot = jnp.where(is_halo, tail - ATOMS, 0)
    near = jnp.where(is_halo, 0, tail)

    def at_ends(row):
        tiles = [row(j) for j in range(AT)]
        return (
            lookup(tiles, head // LANES, head % LANES),
            lookup(tiles, near // LANES, near % LANES),
        )

    ends = [at_ends(lambda j, k=k: table[j, k : k + 1, :]) for k in range(7)]
    head_mass = ends[6][0]
    near_mass = jnp.where(is_halo, 0.0, ends[6][1])

    def to_cols(k, value):
        for t in range(BT):
            col = jnp.sum(jnp.where(eye, value[t : t + 1, :], 0.0), axis=1, keepdims=True)
            cols[k, t * LANES : (t + 1) * LANES, :] = jnp.broadcast_to(col, (LANES, LANES))

    to_cols(0, head.astype(F32))
    to_cols(1, tail.astype(F32))
    to_cols(2, head_mass)
    to_cols(3, near_mass)

    inverse[...] = jnp.zeros((AT + ST, LANES), F32)

    def incidence_rows(t, carry):
        here = pl.ds(pl.multiple_of(t * LANES, LANES), LANES)
        heads = cols[0, here, :]
        tails = cols[1, here, :]
        number = (sub128 + (t * LANES + 1)).astype(F32)
        for j in range(AT + ST):
            atom = (lane128 + j * LANES).astype(F32)
            is_tail = tails == atom
            if j < AT:
                is_head = heads == atom
                incidence[here, j * LANES : (j + 1) * LANES] = (
                    jnp.where(is_head, 1.0, 0.0) - jnp.where(is_tail, 1.0, 0.0)
                ).astype(jnp.bfloat16)
                found = is_head
            else:
                found = is_tail
            inverse[j : j + 1, :] += jnp.sum(
                jnp.where(found, number, 0.0), axis=0, keepdims=True
            )
        return carry

    lax.fori_loop(0, BT, incidence_rows, 0)

    def merge(source, width):
        tiles = []
        for tile in range(ST):
            out = jnp.zeros((width, LANES), F32)
            for b in BLOCKS:
                if b // 8 == tile:
                    out = jnp.where(group8[:width] == b % 8, source[ROW_OF[b]], out)
            tiles.append(out)
        return tiles

    all_of(0, r0_in).wait_recv()
    halo = merge(r0_in, 8)
    slot_tile, slot_lane = slot // LANES, slot % LANES
    tail_data = []
    for k in range(7):
        far = lookup([halo[s][k : k + 1, :] for s in range(ST)], slot_tile, slot_lane)
        tail_data.append(jnp.where(is_halo, far, ends[k][1]))
    head_data = [e[0] for e in ends]

    bond = [head_data[i] - tail_data[i] for i in range(3)]
    length = jnp.maximum(jnp.sqrt(bond[0] * bond[0] + bond[1] * bond[1] + bond[2] * bond[2]), 0.5)
    direction = [b / length for b in bond]
    scale = 1.0 / jnp.sqrt(head_mass + tail_data[6])
    gain = [scale * d for d in direction]
    head_new = [head_data[i] + head_data[3 + i] for i in range(3)]
    tail_new = [tail_data[i] + tail_data[3 + i] for i in range(3)]
    shift = [head_new[i] - tail_new[i] for i in range(3)]
    right = scale * (
        direction[0] * shift[0] + direction[1] * shift[1] + direction[2] * shift[2] - length
    )
    own = 1.0 - head_mass * (gain[0] * gain[0] + gain[1] * gain[1] + gain[2] * gain[2])
    for i in range(3):
        to_cols(4 + i, gain[i])
    rows[0] = head.astype(F32)
    rows[1] = tail.astype(F32)
    for i in range(3):
        rows[2 + i] = gain[i]

    def coupling_rows(t, carry):
        here = pl.ds(pl.multiple_of(t * LANES, LANES), LANES)
        heads, tails = cols[0, here, :], cols[1, here, :]
        masses, near_masses = cols[2, here, :], cols[3, here, :]
        gains = [cols[4 + i, here, :] for i in range(3)]
        for u in range(BT):
            head_row, tail_row = rows[0, u : u + 1, :], rows[1, u : u + 1, :]
            shared = jnp.where(
                tails == head_row, -near_masses, jnp.where(tails == tail_row, near_masses, 0.0)
            ) - jnp.where(heads == tail_row, masses, 0.0)
            dots = (
                gains[0] * rows[2, u : u + 1, :]
                + gains[1] * rows[3, u : u + 1, :]
                + gains[2] * rows[4, u : u + 1, :]
            )
            coupling[here, u * LANES : (u + 1) * LANES] = shared * dots
        return carry

    lax.fori_loop(0, BT, coupling_rows, 0)

    def couple(values):
        for n, value in enumerate(values):
            vec[n] = value
        outs = [[] for _ in values]
        for t in range(BT):
            for n in range(len(values)):
                total = None
                for u in range(BT):
                    part = (
                        coupling[t * LANES : (t + 1) * LANES, u * LANES : (u + 1) * LANES]
                        * vec[n, u : u + 1, :]
                    )
                    total = part if total is None else total + part
                col = jnp.sum(total, axis=1, keepdims=True)
                outs[n].append(jnp.sum(jnp.where(eye, col, 0.0), axis=0, keepdims=True))
        return [own * v - jnp.concatenate(o, axis=0) for v, o in zip(values, outs)]

    def put_kinds(values):
        for k, value in enumerate(values):
            for t in range(BT):
                kinds[t, k : k + 1, :] = value[t : t + 1, :]

    slots = inverse[AT : AT + ST, :].astype(I32)

    def to_slots(values, out):
        width = out.shape[1]
        put_kinds(values)
        for s in range(ST):
            where = jnp.broadcast_to(slots[s : s + 1, :], (width, LANES))
            used = where > 0
            bond_of = jnp.maximum(where - 1, 0)
            tile, lane = bond_of // LANES, bond_of % LANES
            result = jnp.zeros((width, LANES), F32)
            for t in range(BT):
                result = jnp.where(tile == t, take(kinds[t, :width, :], lane), result)
            out[s] = jnp.where(used, result, 0.0)

    unit = jnp.where(is_halo, 1.0, 0.0)
    chain, reach = [right], [unit]
    for _ in range(3):
        nxt = couple([chain[-1], reach[-1]])
        chain.append(nxt[0])
        reach.append(nxt[1])
    zero = jnp.zeros((8, LANES), F32)
    to_slots(gain + reach[1:] + chain[0:2], a_out)
    start(1, lambda b: a_out.at[b // 8], a_in, 1)
    chain.append(couple([chain[-1]])[0])
    to_slots(chain[2:] + [zero], a2_out)
    start(2, lambda b: a2_out.at[b // 8], a2_in, 1)

    atom_bond = inverse[0:16, :].astype(I32)
    parent = lookup(
        [inverse[j : j + 1, :] for j in range(AT)], near // LANES, near % LANES
    ).astype(I32)
    has_parent = jnp.logical_and(parent > 0, jnp.logical_not(is_halo))
    parent = jnp.maximum(parent - 1, 0)
    root = jnp.where(is_halo, slot + 1, 0).astype(F32)
    label = root
    for _ in range(4):
        above = lookup([label[t : t + 1, :] for t in range(BT)], parent // LANES, parent % LANES)
        label = jnp.where(has_parent, above, root)
    bond_at = jnp.maximum(atom_bond - 1, 0)
    atom_label = lookup([label[t : t + 1, :] for t in range(BT)], bond_at // LANES, bond_at % LANES)
    row16 = lax.broadcasted_iota(I32, (16, LANES), 0)
    atom_label = jnp.where(
        jnp.logical_and(atom_bond > 0, row16 < AT), atom_label, 0.0
    ).astype(I32)
    label = label.astype(I32)

    def labelled(tiles, which):
        at = jnp.maximum(which - 1, 0)
        return jnp.where(which > 0, lookup(tiles, at // LANES, at % LANES), 0.0)

    def to_atoms(values):
        weighted = [v * g for v in values for g in gain]
        n = len(weighted)
        height = (n + 7) // 8 * 8
        put_kinds(weighted + [zero] * (height - n))
        full = jnp.concatenate([kinds[t, :height, :] for t in range(BT)], axis=1)
        high = full.astype(jnp.bfloat16)
        rest = full - high.astype(F32)
        mid = rest.astype(jnp.bfloat16)
        low = (rest - mid.astype(F32)).astype(jnp.bfloat16)
        total = None
        for part in (low, mid, high):
            product = jnp.dot(part, incidence[...], preferred_element_type=F32)
            total = product if total is None else total + product
        for j in range(AT):
            sums[j, :height, :] = total[:, j * LANES : (j + 1) * LANES]

    base = chain[0] + chain[1] + chain[2] + chain[3] + chain[4]
    grown = [reach[0]]
    for m in range(1, 4):
        grown.append(grown[-1] + reach[m])
    to_atoms([base] + grown)
    moves = []
    for n in range(15):
        at_head, at_near = at_ends(lambda j, n=n: sums[j, n : n + 1, :])
        moves.append(head_mass * at_head - near_mass * at_near)
    for n in range(15):
        for j in range(AT):
            gathered[n, j : j + 1, :] = sums[j, n : n + 1, :]
        gathered[n, AT:16, :] = jnp.zeros((16 - AT, LANES), F32)

    def by_kind(tiles, count):
        for s in range(ST):
            kinds[s, 0 : tiles[s].shape[0], :] = tiles[s]
        return [
            jnp.concatenate([kinds[s, k : k + 1, :] for s in range(ST)], axis=0)
            for k in range(count)
        ]

    def over_senders(values):
        lines = [jnp.sum(v, axis=0, keepdims=True) for v in values]
        lines += [jnp.zeros((1, LANES), F32)] * (-len(lines) % 8)
        block = jnp.concatenate(lines, axis=0)
        for step in (64, 32, 16):
            block = block + pltpu.roll(block, step, axis=1)
        return block

    own_mass = mine[6:7, :]

    def solve(sums_of, squares):
        found = []
        for k in range(5):
            now = []
            for i in range(3):
                total = sums_of(k, i)
                for j in range(k):
                    for m in range(3):
                        total = total + squares(k - 1 - j, i, m) * found[j][m]
                now.append(-own_mass * total)
            found.append(now)
        return found

    all_of(1, a_in).wait_recv()
    all_of(2, a2_in).wait_recv()
    first = by_kind(merge(a_in, 8), 8)
    second = by_kind(merge(a2_in, 4), 3)
    far_gain, far_reach, far_chain = first[0:3], first[3:6], first[6:8] + second
    lists = [far_gain[i] * far_chain[k] for k in range(5) for i in range(3)]
    squares_of = [far_gain[i] * far_gain[m] for i, m in PAIRS]
    lists += squares_of + [q * far_reach[n] for n in range(3) for q in squares_of]
    block = over_senders(lists)

    def squares(power, i, m):
        at = 15 + power * 6 + PAIRS.index((min(i, m), max(i, m)))
        return block[at : at + 1, :]

    found = solve(lambda k, i: block[3 * k + i : 3 * k + i + 1, :], squares)
    sent_total = [found[0][i] + found[1][i] + found[2][i] + found[3][i] + found[4][i] for i in range(3)]
    for k in range(4):
        z = sum(far_gain[i] * found[k][i] for i in range(3))
        for s in range(ST):
            b_out[s, k : k + 1, :] = z[s : s + 1, :]
    for i in range(3):
        moved = mine[i : i + 1, :] + mine[3 + i : 4 + i, :] - sent_total[i]
        for s in range(ST):
            b_out[s, 4 + i : 5 + i, :] = moved
    for s in range(ST):
        b_out[s, 7:8, :] = jnp.zeros((1, LANES), F32)
    start(3, lambda b: b_out.at[b // 8], b_in, -1)

    all_of(3, b_in).wait_recv()
    back = merge(b_in, 8)

    def kind_rows(tiles, k):
        return [tiles[s][k : k + 1, :] for s in range(ST)]

    z = [labelled(kind_rows(back, k), label) for k in range(4)]
    far_pos = [labelled(kind_rows(back, 4 + i), label) for i in range(3)]
    sol_one = base
    for j in range(4):
        sol_one = sol_one + z[j] * grown[3 - j]
    current = None
    for i in range(3):
        ahead = head_new[i] - jnp.where(is_halo, far_pos[i], tail_new[i])
        step = moves[i]
        for j in range(4):
            step = step + z[j] * moves[3 * (1 + 3 - j) + i]
        stretch = ahead - step
        current = stretch * stretch if current is None else current + stretch * stretch
    target = jnp.sqrt(jnp.maximum(2.0 * length * length - current, 0.5 * length * length))
    chain_two = [scale * (length - target)]
    for _ in range(4):
        chain_two.append(couple([chain_two[-1]])[0])
    to_slots(chain_two + [zero] * 3, c_out)
    start(4, lambda b: c_out.at[b // 8], c_in, 1)

    base_two = chain_two[0] + chain_two[1] + chain_two[2] + chain_two[3] + chain_two[4]
    to_atoms([base_two])
    mass_atoms = jnp.concatenate(
        [table[j, 6:7, :] for j in range(AT)] + [jnp.zeros((16 - AT, LANES), F32)], axis=0
    )
    still = []
    for i in range(3):
        spread_base = jnp.concatenate(
            [gathered[i, j : j + 1, :] + sums[j, i : i + 1, :] for j in range(AT)]
            + [jnp.zeros((16 - AT, LANES), F32)],
            axis=0,
        )
        start_pos = jnp.concatenate(
            [table[j, i : i + 1, :] + table[j, 3 + i : 4 + i, :] for j in range(AT)]
            + [jnp.zeros((16 - AT, LANES), F32)],
            axis=0,
        )
        still.append(start_pos - mass_atoms * spread_base)
    trees = [[mass_atoms * gathered[3 * (1 + n) + i] for i in range(3)] for n in range(4)]
    number16 = row16 * LANES + lax.broadcasted_iota(I32, (16, LANES), 1)
    which = jnp.zeros((16, LANES), I32)
    for e in range(SEND):
        which = jnp.where(number16 == sent8[0:1, e : e + 1], e + 1, which)

    all_of(4, c_in).wait_recv()
    far_two = by_kind(merge(c_in, 8), 5)
    block_two = over_senders([far_gain[i] * far_two[k] for k in range(5) for i in range(3)])
    found_two = solve(lambda k, i: block_two[3 * k + i : 3 * k + i + 1, :], squares)
    for k in range(4):
        z_two = sum(far_gain[i] * found_two[k][i] for i in range(3))
        for s in range(ST):
            d_out[s, k : k + 1, :] = z_two[s : s + 1, :]
    start(5, lambda b: d_out.at[b // 8], d_in, -1)

    for i in range(3):
        total = sent_total[i]
        for k in range(5):
            total = total + found_two[k][i]
        own_move = take(jnp.broadcast_to(total, (16, LANES)), jnp.maximum(which - 1, 0))
        still[i] = still[i] - jnp.where(which > 0, own_move, 0.0)

    all_of(5, d_in).wait_recv()
    last = merge(d_in, 4)
    result = sol_one + base_two
    for j in range(4):
        result = result + labelled(kind_rows(last, j), label) * grown[3 - j]
    for t in range(BT):
        mult_ref[:, t * LANES : (t + 1) * LANES] = result[t : t + 1, :]
    both = [[back[s][k : k + 1, :] + last[s][k : k + 1, :] for s in range(ST)] for k in range(4)]
    for j in range(4):
        z_atom = labelled(both[j], atom_label)
        for i in range(3):
            still[i] = still[i] - z_atom * trees[3 - j][i]
    for i in range(3):
        for j in range(AT):
            new_ref[i, :, j * LANES : (j + 1) * LANES] = still[i][j : j + 1, :]

    for stage, target in enumerate((r0_in, a_in, a2_in, b_in, c_in, d_in)):
        all_of(stage, target).wait_send()


def solution(mesh):
    sizes = tuple(mesh.shape[n] for n in ("gx", "gy", "gz"))

    def per_device(old_pos, displacement, inv_mass, bond_head, bond_tail, send_list):
        near = len(BLOCKS)
        vmem = pl.BlockSpec(memory_space=pltpu.VMEM)
        new_pos, multipliers = pl.pallas_call(
            functools.partial(kernel, sizes),
            out_shape=(
                jax.ShapeDtypeStruct((3, 1, ATOMS), F32),
                jax.ShapeDtypeStruct((1, BONDS), F32),
            ),
            in_specs=[vmem] * 6,
            out_specs=(vmem, vmem),
            scratch_shapes=[
                pltpu.VMEM((AT, 8, LANES), F32),
                pltpu.VMEM((2, 8, LANES), I32),
                pltpu.VMEM((7, BONDS, LANES), F32),
                pltpu.VMEM((BONDS, ATOMS), jnp.bfloat16),
                pltpu.VMEM((BONDS, BONDS), F32),
                pltpu.VMEM((AT + ST, LANES), F32),
                pltpu.VMEM((2, 8, LANES), F32),
                pltpu.VMEM((5, 8, LANES), F32),
                pltpu.VMEM((AT, 16, LANES), F32),
                pltpu.VMEM((8, 16, LANES), F32),
                pltpu.VMEM((15, 16, LANES), F32),
                pltpu.VMEM((8, LANES), F32),
                pltpu.VMEM((ST, 8, LANES), F32),
                pltpu.VMEM((ST, 4, LANES), F32),
                pltpu.VMEM((ST, 8, LANES), F32),
                pltpu.VMEM((ST, 8, LANES), F32),
                pltpu.VMEM((ST, 4, LANES), F32),
                pltpu.VMEM((near, 8, LANES), F32),
                pltpu.VMEM((near, 8, LANES), F32),
                pltpu.VMEM((near, 4, LANES), F32),
                pltpu.VMEM((near, 8, LANES), F32),
                pltpu.VMEM((near, 8, LANES), F32),
                pltpu.VMEM((near, 4, LANES), F32),
                pltpu.SemaphoreType.DMA((6,)),
                pltpu.SemaphoreType.DMA((6,)),
            ],
            compiler_params=pltpu.CompilerParams(collective_id=0, has_side_effects=True),
        )(
            old_pos.reshape(3, 1, ATOMS),
            displacement.reshape(3, 1, ATOMS),
            inv_mass.reshape(1, ATOMS),
            bond_head.reshape(1, BONDS),
            bond_tail.reshape(1, BONDS),
            send_list.reshape(1, SEND),
        )
        return new_pos.reshape(old_pos.shape), multipliers.reshape(bond_head.shape)

    return jax.shard_map(
        per_device,
        mesh=mesh,
        in_specs=(
            P(None, "gx", "gy", "gz", None),
            P(None, "gx", "gy", "gz", None),
            P("gx", "gy", "gz", None),
            P("gx", "gy", "gz", None),
            P("gx", "gy", "gz", None),
            P("gx", "gy", "gz", None),
        ),
        out_specs=(P(None, "gx", "gy", "gz", None), P("gx", "gy", "gz", None)),
        check_vma=False,
    )
```

```python
import functools

import jax
import jax.numpy as jnp
from jax import lax
from jax.experimental import pallas as pl
from jax.experimental.pallas import tpu as pltpu
from jax.sharding import PartitionSpec as P

MESH = pl.DeviceIdType.MESH
ATOMS = 1536
BONDS = 1024
SEND = 16
LANES = 128
AT = ATOMS // LANES
BT = BONDS // LANES
ST = 4
BLOCKS = [b for b in range(27) if b != 13]
ROW_OF = {b: n for n, b in enumerate(BLOCKS)}
F32 = jnp.float32
I32 = jnp.int32
PAIRS = [(0, 0), (0, 1), (0, 2), (1, 1), (1, 2), (2, 2)]


def take(rows, lane):
    numbers = lax.GatherDimensionNumbers(
        offset_dims=(),
        collapsed_slice_dims=(1,),
        start_index_map=(1,),
        operand_batching_dims=(0,),
        start_indices_batching_dims=(0,),
    )
    return lax.gather(
        rows, lane[..., None], numbers, (1, 1), mode=lax.GatherScatterMode.PROMISE_IN_BOUNDS
    )


def lookup(tiles, tile, lane):
    out = jnp.zeros(lane.shape, F32)
    for j, row in enumerate(tiles):
        out = jnp.where(tile == j, take(jnp.broadcast_to(row, lane.shape), lane), out)
    return out


def kernel(
    sizes,
    old_ref,
    move_ref,
    mass_ref,
    head_ref,
    tail_ref,
    send_ref,
    new_ref,
    mult_ref,
    table,
    idx,
    cols,
    incidence,
    trees_of,
    coupling,
    inverse,
    vec,
    rows,
    sums,
    kinds,
    gathered,
    r0_out,
    a_out,
    b_out,
    c_out,
    d_out,
    r0_in,
    a_in,
    b_in,
    c_in,
    d_in,
    send_sem,
    recv_sem,
):
    names = ("gx", "gy", "gz")
    me = [lax.axis_index(n) for n in names]

    def device(block, sign):
        offs = (block // 9 - 1, block // 3 % 3 - 1, block % 3 - 1)
        return tuple(lax.rem(m + sign * o + n, n) for m, o, n in zip(me, offs, sizes))

    barrier = pltpu.get_barrier_semaphore()
    for b in BLOCKS:
        pl.semaphore_signal(barrier, inc=1, device_id=device(b, 1), device_id_type=MESH)

    def start(stage, source, target, sign):
        for b in BLOCKS:
            pltpu.make_async_remote_copy(
                src_ref=source(b),
                dst_ref=target.at[ROW_OF[b]],
                send_sem=send_sem.at[stage],
                recv_sem=recv_sem.at[stage],
                device_id=device(b, sign),
                device_id_type=MESH,
            ).start()

    def all_of(stage, target):
        return pltpu.make_async_remote_copy(
            src_ref=target,
            dst_ref=target,
            send_sem=send_sem.at[stage],
            recv_sem=recv_sem.at[stage],
            device_id=device(0, 1),
            device_id_type=MESH,
        )

    lane8 = lax.broadcasted_iota(I32, (8, LANES), 1)
    group8 = lane8 // SEND
    sub128 = lax.broadcasted_iota(I32, (LANES, LANES), 0)
    lane128 = lax.broadcasted_iota(I32, (LANES, LANES), 1)
    eye = sub128 == lane128

    for j in range(AT):
        cut = pl.ds(j * LANES, LANES)
        for i in range(3):
            table[j, i : i + 1, :] = old_ref[i, :, cut]
            table[j, 3 + i : 4 + i, :] = move_ref[i, :, cut]
        table[j, 6:7, :] = mass_ref[:, cut]
        table[j, 7:8, :] = jnp.zeros((1, LANES), F32)
    sent8 = jnp.broadcast_to(
        jnp.concatenate([send_ref[...]] * (LANES // SEND), axis=1), (8, LANES)
    )
    mine = jnp.zeros((8, LANES), F32)
    for j in range(AT):
        mine = jnp.where(sent8 // LANES == j, take(table[j], sent8 % LANES), mine)
    r0_out[...] = mine
    pl.semaphore_wait(barrier, len(BLOCKS))
    start(0, lambda b: r0_out, r0_in, -1)

    for t in range(BT):
        cut = pl.ds(t * LANES, LANES)
        idx[0, t : t + 1, :] = head_ref[:, cut]
        idx[1, t : t + 1, :] = tail_ref[:, cut]
    head = idx[0]
    tail = idx[1]
    is_halo = tail >= ATOMS
    slot = jnp.where(is_halo, tail - ATOMS, 0)
    near = jnp.where(is_halo, 0, tail)

    def at_ends(row):
        tiles = [row(j) for j in range(AT)]
        return (
            lookup(tiles, head // LANES, head % LANES),
            lookup(tiles, near // LANES, near % LANES),
        )

    ends = [at_ends(lambda j, k=k: table[j, k : k + 1, :]) for k in range(7)]
    head_mass = ends[6][0]
    near_mass = jnp.where(is_halo, 0.0, ends[6][1])
    head_data = [e[0] for e in ends]
    head_new = [head_data[i] + head_data[3 + i] for i in range(3)]

    def to_cols(k, value):
        for t in range(BT):
            col = jnp.sum(jnp.where(eye, value[t : t + 1, :], 0.0), axis=1, keepdims=True)
            cols[k, t * LANES : (t + 1) * LANES, :] = jnp.broadcast_to(col, (LANES, LANES))

    to_cols(0, head.astype(F32))
    to_cols(1, tail.astype(F32))

    def geometry(ahead, behind, mass, ahead_new, behind_new):
        bond = [p - q for p, q in zip(ahead, behind)]
        length = jnp.maximum(
            jnp.sqrt(bond[0] * bond[0] + bond[1] * bond[1] + bond[2] * bond[2]), 0.5
        )
        direction = [b / length for b in bond]
        scale = 1.0 / jnp.sqrt(mass)
        shift = [p - q for p, q in zip(ahead_new, behind_new)]
        right = scale * (
            direction[0] * shift[0] + direction[1] * shift[1] + direction[2] * shift[2] - length
        )
        return length, scale, [scale * d for d in direction], right

    near_data = [e[1] for e in ends]
    _, _, tree_gain, tree_right = geometry(
        head_data[0:3],
        near_data[0:3],
        head_mass + near_data[6],
        head_new,
        [near_data[i] + near_data[3 + i] for i in range(3)],
    )
    tree_gain = [jnp.where(is_halo, 0.0, g) for g in tree_gain]
    tree_right = jnp.where(is_halo, 0.0, tree_right)

    inverse[...] = jnp.zeros((AT + ST, LANES), F32)
    kinds[...] = jnp.zeros(kinds.shape, F32)

    def incidence_rows(t, carry):
        here = pl.ds(pl.multiple_of(t * LANES, LANES), LANES)
        heads = cols[0, here, :]
        tails = cols[1, here, :]
        number = (sub128 + (t * LANES + 1)).astype(F32)
        for j in range(AT + ST):
            atom = (lane128[0:1] + j * LANES).astype(F32)
            is_tail = tails == atom
            if j < AT:
                found = heads == atom
                incidence[here, j * LANES : (j + 1) * LANES] = jnp.where(
                    found, 1.0, jnp.where(is_tail, -1.0, 0.0)
                ).astype(jnp.bfloat16)
            else:
                found = is_tail
            inverse[j : j + 1, :] += jnp.sum(
                jnp.where(found, number, 0.0), axis=0, keepdims=True
            )
        return carry

    lax.fori_loop(0, BT, incidence_rows, 0)

    parent = lookup(
        [inverse[j : j + 1, :] for j in range(AT)], near // LANES, near % LANES
    ).astype(I32)
    has_parent = jnp.logical_and(parent > 0, jnp.logical_not(is_halo))
    parent = jnp.maximum(parent - 1, 0)
    root = jnp.where(is_halo, slot + 1, 0).astype(F32)

    def climb(label):
        above = lookup([label[t : t + 1, :] for t in range(BT)], parent // LANES, parent % LANES)
        return jnp.where(has_parent, above, root)

    def put_kinds(values):
        for k, value in enumerate(values):
            for t in range(BT):
                kinds[t, k : k + 1, :] = value[t : t + 1, :]

    def times_ones(values, matrix):
        height = (len(values) + 15) // 16 * 16
        put_kinds(values)
        full = jnp.concatenate([kinds[t, :height, :] for t in range(BT)], axis=1)
        high = full.astype(jnp.bfloat16)
        rest = full - high.astype(F32)
        mid = rest.astype(jnp.bfloat16)
        low = (rest - mid.astype(F32)).astype(jnp.bfloat16)
        parts = jnp.concatenate([high, mid, low], axis=0)
        product = jnp.dot(parts, matrix, preferred_element_type=F32)
        return product[:height] + (product[height : 2 * height] + product[2 * height :])

    def to_atoms(weighted):
        total = times_ones(weighted, incidence[...])
        height = (len(weighted) + 7) // 8 * 8
        for j in range(AT):
            sums[j, :height, :] = total[:height, j * LANES : (j + 1) * LANES]

    def difference(n):
        at_head, at_near = at_ends(lambda j: sums[j, n : n + 1, :])
        return head_mass * at_head - near_mass * at_near

    label_one = climb(root)
    child = jnp.logical_and(label_one > 0.0, jnp.logical_not(is_halo))
    label_two = climb(label_one)
    start_of = [jnp.where(child, g, 0.0) for g in tree_gain]
    to_atoms(
        [tree_right * g for g in tree_gain]
        + [start_of[i] * tree_gain[m] for i, m in PAIRS]
    )
    diffs = [difference(n) for n in range(9)]
    tree_next = tree_right - sum(tree_gain[i] * diffs[i] for i in range(3))
    start_next = []
    for i in range(3):
        start_next.append(
            start_of[i]
            - sum(
                tree_gain[m] * diffs[3 + PAIRS.index((min(i, m), max(i, m)))] for m in range(3)
            )
        )
    to_cols(2, label_two)
    for s in range(ST):
        number = (lane128[0:1] + (s * LANES + 1)).astype(F32)
        trees_of[:, s * LANES : (s + 1) * LANES] = jnp.where(cols[2] == number, 1.0, 0.0).astype(
            jnp.bfloat16
        )
    to_atoms([tree_next * g for g in tree_gain])
    diffs = [difference(n) for n in range(3)]
    tree_last = tree_next - sum(tree_gain[i] * diffs[i] for i in range(3))
    tree_sums = times_ones(
        [start_of[i] * start_of[m] for i, m in PAIRS]
        + [start_of[i] * start_next[m] for i, m in PAIRS]
        + [start_next[i] * start_next[m] for i, m in PAIRS]
        + [y * tree_right for y in start_of]
        + [y * tree_next for y in start_of]
        + [y * tree_next for y in start_next]
        + [y * tree_last for y in start_next],
        trees_of[...],
    )
    slots = inverse[AT : AT + ST, :].astype(I32)
    slot_bond = jnp.maximum(slots - 1, 0)
    slot_head = lookup(
        [head[t : t + 1, :].astype(F32) for t in range(BT)],
        slot_bond // LANES,
        slot_bond % LANES,
    ).astype(I32)
    for s in range(ST):
        at = jnp.broadcast_to(slot_head[s : s + 1, :], (8, LANES))
        used = jnp.broadcast_to(slots[s : s + 1, :], (8, LANES)) > 0
        atoms = jnp.zeros((8, LANES), F32)
        for j in range(AT):
            atoms = jnp.where(at // LANES == j, take(table[j], at % LANES), atoms)
        groups = [tree_sums[8 * n : 8 * n + 8, s * LANES : (s + 1) * LANES] for n in range(4)]
        groups.append(jnp.where(used, atoms, 0.0))
        turned = [pltpu.roll(g, SEND * n, axis=1) if n else g for n, g in enumerate(groups)]
        for b in BLOCKS:
            if b // 8 == s:
                out = turned[0]
                for n in range(1, len(turned)):
                    out = jnp.where(group8 == (b + n) % 8, turned[n], out)
                a_out[ROW_OF[b]] = out
    start(1, lambda b: a_out.at[ROW_OF[b]], a_in, 1)

    def merge(source, width, turn=0):
        tiles = []
        for tile in range(ST):
            out = jnp.zeros((width, LANES), F32)
            for b in BLOCKS:
                if b // 8 == tile:
                    out = jnp.where(group8[:width] == (b + turn) % 8, source[ROW_OF[b]], out)
            if turn:
                out = pltpu.roll(out, LANES - SEND * turn, axis=1)
            tiles.append(out)
        return tiles

    all_of(0, r0_in).wait_recv()
    halo = merge(r0_in, 8)
    slot_tile, slot_lane = slot // LANES, slot % LANES
    tail_data = []
    for k in range(7):
        far = lookup([halo[s][k : k + 1, :] for s in range(ST)], slot_tile, slot_lane)
        tail_data.append(jnp.where(is_halo, far, near_data[k]))
    tail_new = [tail_data[i] + tail_data[3 + i] for i in range(3)]
    length, scale, gain, right = geometry(
        head_data[0:3], tail_data[0:3], head_mass + tail_data[6], head_new, tail_new
    )
    own = 1.0 - head_mass * (gain[0] * gain[0] + gain[1] * gain[1] + gain[2] * gain[2])
    to_cols(2, head_mass)
    to_cols(3, near_mass)
    for i in range(3):
        to_cols(4 + i, gain[i])
    rows[0] = head.astype(F32)
    rows[1] = tail.astype(F32)
    for i in range(3):
        rows[2 + i] = gain[i]

    def coupling_rows(t, carry):
        here = pl.ds(pl.multiple_of(t * LANES, LANES), LANES)
        heads, tails = cols[0, here, :], cols[1, here, :]
        masses, near_masses = cols[2, here, :], cols[3, here, :]
        gains = [cols[4 + i, here, :] for i in range(3)]
        for u in range(BT):
            head_row, tail_row = rows[0, u : u + 1, :], rows[1, u : u + 1, :]
            shared = jnp.where(
                tails == head_row, -near_masses, jnp.where(tails == tail_row, near_masses, 0.0)
            ) - jnp.where(heads == tail_row, masses, 0.0)
            dots = (
                gains[0] * rows[2, u : u + 1, :]
                + gains[1] * rows[3, u : u + 1, :]
                + gains[2] * rows[4, u : u + 1, :]
            )
            coupling[here, u * LANES : (u + 1) * LANES] = shared * dots
        return carry

    lax.fori_loop(0, BT, coupling_rows, 0)

    def couple(values):
        for n, value in enumerate(values):
            vec[n] = value
        outs = [[] for _ in values]
        for t in range(BT):
            for n in range(len(values)):
                total = None
                for u in range(BT):
                    part = (
                        coupling[t * LANES : (t + 1) * LANES, u * LANES : (u + 1) * LANES]
                        * vec[n, u : u + 1, :]
                    )
                    total = part if total is None else total + part
                col = jnp.sum(total, axis=1, keepdims=True)
                outs[n].append(jnp.sum(jnp.where(eye, col, 0.0), axis=0, keepdims=True))
        return [own * v - jnp.concatenate(o, axis=0) for v, o in zip(values, outs)]

    def by_kind(tiles, count):
        for s in range(ST):
            kinds[s, 0 : tiles[s].shape[0], :] = tiles[s]
        return [
            jnp.concatenate([kinds[s, k : k + 1, :] for s in range(ST)], axis=0)
            for k in range(count)
        ]

    def over_senders(values):
        lines = [jnp.sum(v, axis=0, keepdims=True) for v in values]
        lines += [jnp.zeros((1, LANES), F32)] * (-len(lines) % 8)
        block = jnp.concatenate(lines, axis=0)
        for step in (64, 32, 16):
            block = block + pltpu.roll(block, step, axis=1)
        return block

    own_mass = mine[6:7, :]

    def solve(sums_of, squares):
        found = []
        for k in range(5):
            now = []
            for i in range(3):
                total = sums_of(k, i)
                for j in range(k):
                    for m in range(3):
                        total = total + squares(k - 1 - j, i, m) * found[j][m]
                now.append(-own_mass * total)
            found.append(now)
        return found

    all_of(1, a_in).wait_recv()
    far = []
    for n in range(5):
        far += by_kind(merge(a_in, 8, n), 8)
    far_head, far_mass = far[32:38], far[38]
    far_new = [far_head[i] + far_head[3 + i] for i in range(3)]
    used = far_mass > 0.0
    _, _, far_gain, far_right = geometry(
        far_head[0:3],
        [mine[i : i + 1, :] for i in range(3)],
        far_mass + own_mass,
        far_new,
        [mine[i : i + 1, :] + mine[3 + i : 4 + i, :] for i in range(3)],
    )
    far_gain = [jnp.where(used, g, 0.0) for g in far_gain]
    far_right = jnp.where(used, far_right, 0.0)
    pull = [far_mass * g for g in far_gain]
    far_own = 1.0 - (pull[0] * far_gain[0] + pull[1] * far_gain[1] + pull[2] * far_gain[2])
    turn = []
    for power in range(3):
        form = far[6 * power : 6 * power + 6]
        turn.append(
            sum(
                pull[i] * sum(pull[m] * form[PAIRS.index((min(i, m), max(i, m)))] for m in range(3))
                for i in range(3)
            )
        )
    feed = [sum(pull[i] * far[18 + 3 * k + i] for i in range(3)) for k in range(4)]
    far_chain = [far_right]
    for k in range(4):
        value = far_own * far_chain[k] + feed[k]
        for j in range(k):
            value = value + turn[k - 1 - j] * far_chain[j]
        far_chain.append(value)
    far_reach = [far_own]
    far_reach.append(far_own * far_own + turn[0])
    far_reach.append(far_own * far_reach[1] + turn[0] * far_own + turn[1])
    lists = [far_gain[i] * far_chain[k] for k in range(5) for i in range(3)]
    squares_of = [far_gain[i] * far_gain[m] for i, m in PAIRS]
    lists += squares_of + [q * far_reach[n] for n in range(3) for q in squares_of]
    block = over_senders(lists)

    def squares(power, i, m):
        at = 15 + power * 6 + PAIRS.index((min(i, m), max(i, m)))
        return block[at : at + 1, :]

    found = solve(lambda k, i: block[3 * k + i : 3 * k + i + 1, :], squares)
    sent_total = [found[0][i] + found[1][i] + found[2][i] + found[3][i] + found[4][i] for i in range(3)]
    for k in range(4):
        z = sum(far_gain[i] * found[k][i] for i in range(3))
        for s in range(ST):
            b_out[s, k : k + 1, :] = z[s : s + 1, :]
    for i in range(3):
        moved = mine[i : i + 1, :] + mine[3 + i : 4 + i, :] - sent_total[i]
        for s in range(ST):
            b_out[s, 4 + i : 5 + i, :] = moved
    for s in range(ST):
        b_out[s, 7:8, :] = jnp.zeros((1, LANES), F32)
    start(3, lambda b: b_out.at[b // 8], b_in, -1)


    label = climb(climb(label_two))
    atom_bond = inverse[0:16, :].astype(I32)
    bond_at = jnp.maximum(atom_bond - 1, 0)
    atom_label = lookup([label[t : t + 1, :] for t in range(BT)], bond_at // LANES, bond_at % LANES)
    row16 = lax.broadcasted_iota(I32, (16, LANES), 0)
    atom_label = jnp.where(
        jnp.logical_and(atom_bond > 0, row16 < AT), atom_label, 0.0
    ).astype(I32)
    label = label.astype(I32)

    def labelled(tiles, which):
        at = jnp.maximum(which - 1, 0)
        return jnp.where(which > 0, lookup(tiles, at // LANES, at % LANES), 0.0)

    unit = jnp.where(is_halo, 1.0, 0.0)
    chain, reach = [right], [unit]
    for _ in range(3):
        nxt = couple([chain[-1], reach[-1]])
        chain.append(nxt[0])
        reach.append(nxt[1])
    chain.append(couple([chain[-1]])[0])
    base = chain[0] + chain[1] + chain[2] + chain[3] + chain[4]
    grown = [reach[0]]
    for m in range(1, 4):
        grown.append(grown[-1] + reach[m])
    to_atoms([v * g for v in [base] + grown for g in gain])
    moves = []
    for n in range(15):
        moves.append(difference(n))
    for n in range(15):
        for j in range(AT):
            gathered[n, j : j + 1, :] = sums[j, n : n + 1, :]
        gathered[n, AT:16, :] = jnp.zeros((16 - AT, LANES), F32)

    all_of(3, b_in).wait_recv()
    back = merge(b_in, 8)

    def kind_rows(tiles, k):
        return [tiles[s][k : k + 1, :] for s in range(ST)]

    z = [labelled(kind_rows(back, k), label) for k in range(4)]
    far_pos = [labelled(kind_rows(back, 4 + i), label) for i in range(3)]
    sol_one = base
    for j in range(4):
        sol_one = sol_one + z[j] * grown[3 - j]
    current = None
    for i in range(3):
        ahead = head_new[i] - jnp.where(is_halo, far_pos[i], tail_new[i])
        step = moves[i]
        for j in range(4):
            step = step + z[j] * moves[3 * (1 + 3 - j) + i]
        stretch = ahead - step
        current = stretch * stretch if current is None else current + stretch * stretch
    target = jnp.sqrt(jnp.maximum(2.0 * length * length - current, 0.5 * length * length))
    chain_two = [scale * (length - target)]
    for _ in range(2):
        chain_two.append(couple([chain_two[-1]])[0])
    tree_sums = times_ones(
        [unit * v for v in chain_two] + [reach[1] * chain_two[2], reach[2] * chain_two[2]],
        trees_of[...],
    )
    for s in range(ST):
        c_out[s] = tree_sums[0:8, s * LANES : (s + 1) * LANES]
    start(4, lambda b: c_out.at[b // 8], c_in, 1)
    for _ in range(2):
        chain_two.append(couple([chain_two[-1]])[0])

    base_two = chain_two[0] + chain_two[1] + chain_two[2] + chain_two[3] + chain_two[4]
    to_atoms([base_two * g for g in gain])
    mass_atoms = jnp.concatenate(
        [table[j, 6:7, :] for j in range(AT)] + [jnp.zeros((16 - AT, LANES), F32)], axis=0
    )
    still = []
    for i in range(3):
        spread_base = jnp.concatenate(
            [gathered[i, j : j + 1, :] + sums[j, i : i + 1, :] for j in range(AT)]
            + [jnp.zeros((16 - AT, LANES), F32)],
            axis=0,
        )
        start_pos = jnp.concatenate(
            [table[j, i : i + 1, :] + table[j, 3 + i : 4 + i, :] for j in range(AT)]
            + [jnp.zeros((16 - AT, LANES), F32)],
            axis=0,
        )
        still.append(start_pos - mass_atoms * spread_base)
    trees = [[mass_atoms * gathered[3 * (1 + n) + i] for i in range(3)] for n in range(4)]
    number16 = row16 * LANES + lax.broadcasted_iota(I32, (16, LANES), 1)
    which = jnp.zeros((16, LANES), I32)
    for e in range(SEND):
        which = jnp.where(number16 == sent8[0:1, e : e + 1], e + 1, which)

    all_of(4, c_in).wait_recv()
    far_two = by_kind(merge(c_in, 8), 5)
    block_two = over_senders([far_gain[i] * far_two[k] for k in range(5) for i in range(3)])
    found_two = solve(lambda k, i: block_two[3 * k + i : 3 * k + i + 1, :], squares)
    for k in range(4):
        z_two = sum(far_gain[i] * found_two[k][i] for i in range(3))
        for s in range(ST):
            d_out[s, k : k + 1, :] = z_two[s : s + 1, :]
    start(5, lambda b: d_out.at[b // 8], d_in, -1)

    for i in range(3):
        total = sent_total[i]
        for k in range(5):
            total = total + found_two[k][i]
        own_move = take(jnp.broadcast_to(total, (16, LANES)), jnp.maximum(which - 1, 0))
        still[i] = still[i] - jnp.where(which > 0, own_move, 0.0)

    all_of(5, d_in).wait_recv()
    last = merge(d_in, 4)
    result = sol_one + base_two
    for j in range(4):
        result = result + labelled(kind_rows(last, j), label) * grown[3 - j]
    for t in range(BT):
        mult_ref[:, t * LANES : (t + 1) * LANES] = result[t : t + 1, :]
    both = [[back[s][k : k + 1, :] + last[s][k : k + 1, :] for s in range(ST)] for k in range(4)]
    for j in range(4):
        z_atom = labelled(both[j], atom_label)
        for i in range(3):
            still[i] = still[i] - z_atom * trees[3 - j][i]
    for i in range(3):
        for j in range(AT):
            new_ref[i, :, j * LANES : (j + 1) * LANES] = still[i][j : j + 1, :]

    for stage, target in ((0, r0_in), (1, a_in), (3, b_in), (4, c_in), (5, d_in)):
        all_of(stage, target).wait_send()


def solution(mesh):
    sizes = tuple(mesh.shape[n] for n in ("gx", "gy", "gz"))

    def per_device(old_pos, displacement, inv_mass, bond_head, bond_tail, send_list):
        near = len(BLOCKS)
        vmem = pl.BlockSpec(memory_space=pltpu.VMEM)
        new_pos, multipliers = pl.pallas_call(
            functools.partial(kernel, sizes),
            out_shape=(
                jax.ShapeDtypeStruct((3, 1, ATOMS), F32),
                jax.ShapeDtypeStruct((1, BONDS), F32),
            ),
            in_specs=[vmem] * 6,
            out_specs=(vmem, vmem),
            scratch_shapes=[
                pltpu.VMEM((AT, 8, LANES), F32),
                pltpu.VMEM((2, 8, LANES), I32),
                pltpu.VMEM((7, BONDS, LANES), F32),
                pltpu.VMEM((BONDS, ATOMS), jnp.bfloat16),
                pltpu.VMEM((BONDS, ST * LANES), jnp.bfloat16),
                pltpu.VMEM((BONDS, BONDS), F32),
                pltpu.VMEM((AT + ST, LANES), F32),
                pltpu.VMEM((2, 8, LANES), F32),
                pltpu.VMEM((5, 8, LANES), F32),
                pltpu.VMEM((AT, 16, LANES), F32),
                pltpu.VMEM((8, 40, LANES), F32),
                pltpu.VMEM((15, 16, LANES), F32),
                pltpu.VMEM((8, LANES), F32),
                pltpu.VMEM((near, 8, LANES), F32),
                pltpu.VMEM((ST, 8, LANES), F32),
                pltpu.VMEM((ST, 8, LANES), F32),
                pltpu.VMEM((ST, 4, LANES), F32),
                pltpu.VMEM((near, 8, LANES), F32),
                pltpu.VMEM((near, 8, LANES), F32),
                pltpu.VMEM((near, 8, LANES), F32),
                pltpu.VMEM((near, 8, LANES), F32),
                pltpu.VMEM((near, 4, LANES), F32),
                pltpu.SemaphoreType.DMA((6,)),
                pltpu.SemaphoreType.DMA((6,)),
            ],
            compiler_params=pltpu.CompilerParams(collective_id=0, has_side_effects=True),
        )(
            old_pos.reshape(3, 1, ATOMS),
            displacement.reshape(3, 1, ATOMS),
            inv_mass.reshape(1, ATOMS),
            bond_head.reshape(1, BONDS),
            bond_tail.reshape(1, BONDS),
            send_list.reshape(1, SEND),
        )
        return new_pos.reshape(old_pos.shape), multipliers.reshape(bond_head.shape)

    return jax.shard_map(
        per_device,
        mesh=mesh,
        in_specs=(
            P(None, "gx", "gy", "gz", None),
            P(None, "gx", "gy", "gz", None),
            P("gx", "gy", "gz", None),
            P("gx", "gy", "gz", None),
            P("gx", "gy", "gz", None),
            P("gx", "gy", "gz", None),
        ),
        out_specs=(P(None, "gx", "gy", "gz", None), P("gx", "gy", "gz", None)),
        check_vma=False,
    )
```

```python
import functools

import jax
import jax.numpy as jnp
from jax import lax
from jax.experimental import pallas as pl
from jax.experimental.pallas import tpu as pltpu
from jax.sharding import PartitionSpec as P

MESH = pl.DeviceIdType.MESH
ATOMS = 1536
BONDS = 1024
SEND = 16
LANES = 128
AT = ATOMS // LANES
BT = BONDS // LANES
ST = 4
BLOCKS = [b for b in range(27) if b != 13]
ROW_OF = {b: n for n, b in enumerate(BLOCKS)}
F32 = jnp.float32
I32 = jnp.int32
PAIRS = [(0, 0), (0, 1), (0, 2), (1, 1), (1, 2), (2, 2)]


def take(rows, lane):
    numbers = lax.GatherDimensionNumbers(
        offset_dims=(),
        collapsed_slice_dims=(1,),
        start_index_map=(1,),
        operand_batching_dims=(0,),
        start_indices_batching_dims=(0,),
    )
    return lax.gather(
        rows, lane[..., None], numbers, (1, 1), mode=lax.GatherScatterMode.PROMISE_IN_BOUNDS
    )


def lookup(tiles, tile, lane):
    out = jnp.zeros(lane.shape, F32)
    for j, row in enumerate(tiles):
        out = jnp.where(tile == j, take(jnp.broadcast_to(row, lane.shape), lane), out)
    return out


def kernel(
    sizes,
    old_hbm,
    move_hbm,
    mass_hbm,
    head_hbm,
    tail_hbm,
    send_hbm,
    new_ref,
    mult_ref,
    old_ref,
    move_ref,
    mass_ref,
    head_ref,
    tail_ref,
    send_ref,
    load_sem,
    table,
    idx,
    cols,
    incidence,
    trees_of,
    coupling,
    found_by,
    inverse,
    vec,
    rows,
    sums,
    kinds,
    gathered,
    r0_out,
    a_out,
    b_out,
    c_out,
    d_out,
    r0_in,
    a_in,
    b_in,
    c_in,
    d_in,
    send_sem,
    recv_sem,
):
    loads = [
        pltpu.make_async_copy(source, target, load_sem.at[n])
        for n, (source, target) in enumerate(
            (
                (send_hbm, send_ref),
                (old_hbm, old_ref),
                (move_hbm, move_ref),
                (mass_hbm, mass_ref),
                (head_hbm, head_ref),
                (tail_hbm, tail_ref),
            )
        )
    ]
    for load in loads:
        load.start()
    names = ("gx", "gy", "gz")
    me = [lax.axis_index(n) for n in names]

    def device(block, sign):
        offs = (block // 9 - 1, block // 3 % 3 - 1, block % 3 - 1)
        return tuple(lax.rem(m + sign * o + n, n) for m, o, n in zip(me, offs, sizes))

    barrier = pltpu.get_barrier_semaphore()
    for b in BLOCKS:
        pl.semaphore_signal(barrier, inc=1, device_id=device(b, 1), device_id_type=MESH)

    def start(stage, source, target, sign):
        for b in BLOCKS:
            pltpu.make_async_remote_copy(
                src_ref=source(b),
                dst_ref=target.at[ROW_OF[b]],
                send_sem=send_sem.at[stage],
                recv_sem=recv_sem.at[stage],
                device_id=device(b, sign),
                device_id_type=MESH,
            ).start()

    def all_of(stage, target):
        return pltpu.make_async_remote_copy(
            src_ref=target,
            dst_ref=target,
            send_sem=send_sem.at[stage],
            recv_sem=recv_sem.at[stage],
            device_id=device(0, 1),
            device_id_type=MESH,
        )

    lane8 = lax.broadcasted_iota(I32, (8, LANES), 1)
    group8 = lane8 // SEND
    sub128 = lax.broadcasted_iota(I32, (LANES, LANES), 0)
    lane128 = lax.broadcasted_iota(I32, (LANES, LANES), 1)
    eye = sub128 == lane128

    for load in loads:
        load.wait()
    for j in range(AT):
        cut = pl.ds(j * LANES, LANES)
        for i in range(3):
            table[j, i : i + 1, :] = old_ref[i, :, cut]
            table[j, 3 + i : 4 + i, :] = move_ref[i, :, cut]
        table[j, 6:7, :] = mass_ref[:, cut]
        table[j, 7:8, :] = jnp.zeros((1, LANES), F32)
    sent8 = jnp.broadcast_to(
        jnp.concatenate([send_ref[...]] * (LANES // SEND), axis=1), (8, LANES)
    )
    mine = jnp.zeros((8, LANES), F32)
    for j in range(AT):
        mine = jnp.where(sent8 // LANES == j, take(table[j], sent8 % LANES), mine)
    r0_out[...] = mine

    for t in range(BT):
        cut = pl.ds(t * LANES, LANES)
        idx[0, t : t + 1, :] = head_ref[:, cut]
        idx[1, t : t + 1, :] = tail_ref[:, cut]
    head = idx[0]
    tail = idx[1]
    is_halo = tail >= ATOMS
    slot = jnp.where(is_halo, tail - ATOMS, 0)
    near = jnp.where(is_halo, 0, tail)

    def at_ends(row):
        tiles = [row(j) for j in range(AT)]
        return (
            lookup(tiles, head // LANES, head % LANES),
            lookup(tiles, near // LANES, near % LANES),
        )

    ends = [at_ends(lambda j, k=k: table[j, k : k + 1, :]) for k in range(7)]
    head_mass = ends[6][0]
    near_mass = jnp.where(is_halo, 0.0, ends[6][1])
    head_data = [e[0] for e in ends]
    head_new = [head_data[i] + head_data[3 + i] for i in range(3)]

    def to_cols(k, value):
        for t in range(BT):
            col = jnp.sum(jnp.where(eye, value[t : t + 1, :], 0.0), axis=1, keepdims=True)
            cols[k, t * LANES : (t + 1) * LANES, :] = jnp.broadcast_to(col, (LANES, LANES))

    to_cols(0, head.astype(F32))
    to_cols(1, tail.astype(F32))

    def geometry(ahead, behind, mass, ahead_new, behind_new):
        bond = [p - q for p, q in zip(ahead, behind)]
        length = jnp.maximum(
            jnp.sqrt(bond[0] * bond[0] + bond[1] * bond[1] + bond[2] * bond[2]), 0.5
        )
        direction = [b / length for b in bond]
        scale = 1.0 / jnp.sqrt(mass)
        shift = [p - q for p, q in zip(ahead_new, behind_new)]
        right = scale * (
            direction[0] * shift[0] + direction[1] * shift[1] + direction[2] * shift[2] - length
        )
        return length, scale, [scale * d for d in direction], right

    near_data = [e[1] for e in ends]
    _, _, tree_gain, tree_right = geometry(
        head_data[0:3],
        near_data[0:3],
        head_mass + near_data[6],
        head_new,
        [near_data[i] + near_data[3 + i] for i in range(3)],
    )
    tree_gain = [jnp.where(is_halo, 0.0, g) for g in tree_gain]
    tree_right = jnp.where(is_halo, 0.0, tree_right)

    found_by[...] = jnp.zeros(found_by.shape, F32)
    kinds[...] = jnp.zeros(kinds.shape, F32)

    def incidence_rows(t, carry):
        here = pl.ds(pl.multiple_of(t * LANES, LANES), LANES)
        heads = cols[0, here, :]
        tails = cols[1, here, :]
        number = (sub128 + (t * LANES + 1)).astype(F32)
        cuts = [slice(8 * r, 8 * r + 8) for r in range(LANES // 8)]
        for j in range(AT + ST):
            atom = (lane8 + j * LANES).astype(F32)
            number_of = found_by[j]
            parts = []
            for cut in cuts:
                if j < AT:
                    found = heads[cut] == atom
                    parts.append(
                        jnp.where(found, 1.0, jnp.where(tails[cut] == atom, -1.0, 0.0))
                    )
                else:
                    found = tails[cut] == atom
                number_of = jnp.where(found, number[cut], number_of)
            found_by[j] = number_of
            if j < AT:
                incidence[here, j * LANES : (j + 1) * LANES] = jnp.concatenate(
                    parts, axis=0
                ).astype(jnp.bfloat16)
        return carry

    lax.fori_loop(0, 2, incidence_rows, 0)
    pl.semaphore_wait(barrier, len(BLOCKS))
    start(0, lambda b: r0_out, r0_in, -1)
    lax.fori_loop(2, BT, incidence_rows, 0)
    for j in range(AT + ST):
        inverse[j : j + 1, :] = jnp.sum(found_by[j], axis=0, keepdims=True)

    parent = lookup(
        [inverse[j : j + 1, :] for j in range(AT)], near // LANES, near % LANES
    ).astype(I32)
    has_parent = jnp.logical_and(parent > 0, jnp.logical_not(is_halo))
    parent = jnp.maximum(parent - 1, 0)
    root = jnp.where(is_halo, slot + 1, 0).astype(F32)

    def climb(label):
        above = lookup([label[t : t + 1, :] for t in range(BT)], parent // LANES, parent % LANES)
        return jnp.where(has_parent, above, root)

    def put_kinds(values):
        for k, value in enumerate(values):
            for t in range(BT):
                kinds[t, k : k + 1, :] = value[t : t + 1, :]

    def times_ones(values, matrix):
        height = (len(values) + 15) // 16 * 16
        put_kinds(values)
        full = jnp.concatenate([kinds[t, :height, :] for t in range(BT)], axis=1)
        high = full.astype(jnp.bfloat16)
        rest = full - high.astype(F32)
        mid = rest.astype(jnp.bfloat16)
        low = (rest - mid.astype(F32)).astype(jnp.bfloat16)
        parts = jnp.concatenate([high, mid, low], axis=0)
        product = jnp.dot(parts, matrix, preferred_element_type=F32)
        return product[:height] + (product[height : 2 * height] + product[2 * height :])

    def to_atoms(weighted):
        total = times_ones(weighted, incidence[...])
        height = (len(weighted) + 7) // 8 * 8
        for j in range(AT):
            sums[j, :height, :] = total[:height, j * LANES : (j + 1) * LANES]

    def difference(n):
        at_head, at_near = at_ends(lambda j: sums[j, n : n + 1, :])
        return head_mass * at_head - near_mass * at_near

    label_one = climb(root)
    child = jnp.logical_and(label_one > 0.0, jnp.logical_not(is_halo))
    label_two = climb(label_one)
    start_of = [jnp.where(child, g, 0.0) for g in tree_gain]
    to_atoms(
        [tree_right * g for g in tree_gain]
        + [start_of[i] * tree_gain[m] for i, m in PAIRS]
    )
    diffs = [difference(n) for n in range(9)]
    tree_next = tree_right - sum(tree_gain[i] * diffs[i] for i in range(3))
    start_next = []
    for i in range(3):
        start_next.append(
            start_of[i]
            - sum(
                tree_gain[m] * diffs[3 + PAIRS.index((min(i, m), max(i, m)))] for m in range(3)
            )
        )
    to_cols(2, label_two)
    for s in range(ST):
        number = (lane128[0:1] + (s * LANES + 1)).astype(F32)
        trees_of[:, s * LANES : (s + 1) * LANES] = jnp.where(cols[2] == number, 1.0, 0.0).astype(
            jnp.bfloat16
        )
    to_atoms([tree_next * g for g in tree_gain])
    diffs = [difference(n) for n in range(3)]
    tree_last = tree_next - sum(tree_gain[i] * diffs[i] for i in range(3))
    tree_sums = times_ones(
        [start_of[i] * start_of[m] for i, m in PAIRS]
        + [start_of[i] * start_next[m] for i, m in PAIRS]
        + [start_next[i] * start_next[m] for i, m in PAIRS]
        + [y * tree_right for y in start_of]
        + [y * tree_next for y in start_of]
        + [y * tree_next for y in start_next]
        + [y * tree_last for y in start_next],
        trees_of[...],
    )
    slots = inverse[AT : AT + ST, :].astype(I32)
    slot_bond = jnp.maximum(slots - 1, 0)
    slot_head = lookup(
        [head[t : t + 1, :].astype(F32) for t in range(BT)],
        slot_bond // LANES,
        slot_bond % LANES,
    ).astype(I32)
    for s in range(ST):
        at = jnp.broadcast_to(slot_head[s : s + 1, :], (8, LANES))
        used = jnp.broadcast_to(slots[s : s + 1, :], (8, LANES)) > 0
        atoms = jnp.zeros((8, LANES), F32)
        for j in range(AT):
            atoms = jnp.where(at // LANES == j, take(table[j], at % LANES), atoms)
        groups = [tree_sums[8 * n : 8 * n + 8, s * LANES : (s + 1) * LANES] for n in range(4)]
        groups.append(jnp.where(used, atoms, 0.0))
        turned = [pltpu.roll(g, SEND * n, axis=1) if n else g for n, g in enumerate(groups)]
        for b in BLOCKS:
            if b // 8 == s:
                out = turned[0]
                for n in range(1, len(turned)):
                    out = jnp.where(group8 == (b + n) % 8, turned[n], out)
                a_out[ROW_OF[b]] = out
    start(1, lambda b: a_out.at[ROW_OF[b]], a_in, 1)

    def merge(source, width, turn=0):
        tiles = []
        for tile in range(ST):
            out = jnp.zeros((width, LANES), F32)
            for b in BLOCKS:
                if b // 8 == tile:
                    out = jnp.where(group8[:width] == (b + turn) % 8, source[ROW_OF[b]], out)
            if turn:
                out = pltpu.roll(out, LANES - SEND * turn, axis=1)
            tiles.append(out)
        return tiles

    all_of(0, r0_in).wait_recv()
    halo = merge(r0_in, 8)
    slot_tile, slot_lane = slot // LANES, slot % LANES
    tail_data = []
    for k in range(7):
        far = lookup([halo[s][k : k + 1, :] for s in range(ST)], slot_tile, slot_lane)
        tail_data.append(jnp.where(is_halo, far, near_data[k]))
    tail_new = [tail_data[i] + tail_data[3 + i] for i in range(3)]
    length, scale, gain, right = geometry(
        head_data[0:3], tail_data[0:3], head_mass + tail_data[6], head_new, tail_new
    )
    own = 1.0 - head_mass * (gain[0] * gain[0] + gain[1] * gain[1] + gain[2] * gain[2])
    to_cols(2, head_mass)
    to_cols(3, near_mass)
    for i in range(3):
        to_cols(4 + i, gain[i])
    rows[0] = head.astype(F32)
    rows[1] = tail.astype(F32)
    for i in range(3):
        rows[2 + i] = gain[i]

    def coupling_rows(t, carry):
        here = pl.ds(pl.multiple_of(t * LANES, LANES), LANES)
        heads, tails = cols[0, here, :], cols[1, here, :]
        masses, near_masses = cols[2, here, :], cols[3, here, :]
        gains = [cols[4 + i, here, :] for i in range(3)]
        for u in range(BT):
            head_row, tail_row = rows[0, u : u + 1, :], rows[1, u : u + 1, :]
            shared = jnp.where(
                tails == head_row, -near_masses, jnp.where(tails == tail_row, near_masses, 0.0)
            ) - jnp.where(heads == tail_row, masses, 0.0)
            dots = (
                gains[0] * rows[2, u : u + 1, :]
                + gains[1] * rows[3, u : u + 1, :]
                + gains[2] * rows[4, u : u + 1, :]
            )
            coupling[here, u * LANES : (u + 1) * LANES] = shared * dots
        return carry

    lax.fori_loop(0, BT, coupling_rows, 0)

    def couple(values):
        for n, value in enumerate(values):
            vec[n] = value
        outs = [[] for _ in values]
        for t in range(BT):
            for n in range(len(values)):
                total = None
                for u in range(BT):
                    part = (
                        coupling[t * LANES : (t + 1) * LANES, u * LANES : (u + 1) * LANES]
                        * vec[n, u : u + 1, :]
                    )
                    total = part if total is None else total + part
                col = jnp.sum(total, axis=1, keepdims=True)
                outs[n].append(jnp.sum(jnp.where(eye, col, 0.0), axis=0, keepdims=True))
        return [own * v - jnp.concatenate(o, axis=0) for v, o in zip(values, outs)]

    def by_kind(tiles, count):
        for s in range(ST):
            kinds[s, 0 : tiles[s].shape[0], :] = tiles[s]
        return [
            jnp.concatenate([kinds[s, k : k + 1, :] for s in range(ST)], axis=0)
            for k in range(count)
        ]

    def over_senders(values):
        lines = [jnp.sum(v, axis=0, keepdims=True) for v in values]
        lines += [jnp.zeros((1, LANES), F32)] * (-len(lines) % 8)
        block = jnp.concatenate(lines, axis=0)
        for step in (64, 32, 16):
            block = block + pltpu.roll(block, step, axis=1)
        return block

    own_mass = mine[6:7, :]

    def solve(sums_of, squares):
        found = []
        for k in range(5):
            now = []
            for i in range(3):
                total = sums_of(k, i)
                for j in range(k):
                    for m in range(3):
                        total = total + squares(k - 1 - j, i, m) * found[j][m]
                now.append(-own_mass * total)
            found.append(now)
        return found

    all_of(1, a_in).wait_recv()
    far = []
    for n in range(5):
        far += by_kind(merge(a_in, 8, n), 8)
    far_head, far_mass = far[32:38], far[38]
    far_new = [far_head[i] + far_head[3 + i] for i in range(3)]
    used = far_mass > 0.0
    _, _, far_gain, far_right = geometry(
        far_head[0:3],
        [mine[i : i + 1, :] for i in range(3)],
        far_mass + own_mass,
        far_new,
        [mine[i : i + 1, :] + mine[3 + i : 4 + i, :] for i in range(3)],
    )
    far_gain = [jnp.where(used, g, 0.0) for g in far_gain]
    far_right = jnp.where(used, far_right, 0.0)
    pull = [far_mass * g for g in far_gain]
    far_own = 1.0 - (pull[0] * far_gain[0] + pull[1] * far_gain[1] + pull[2] * far_gain[2])
    turn = []
    for power in range(3):
        form = far[6 * power : 6 * power + 6]
        turn.append(
            sum(
                pull[i] * sum(pull[m] * form[PAIRS.index((min(i, m), max(i, m)))] for m in range(3))
                for i in range(3)
            )
        )
    feed = [sum(pull[i] * far[18 + 3 * k + i] for i in range(3)) for k in range(4)]
    far_chain = [far_right]
    for k in range(4):
        value = far_own * far_chain[k] + feed[k]
        for j in range(k):
            value = value + turn[k - 1 - j] * far_chain[j]
        far_chain.append(value)
    far_reach = [far_own]
    far_reach.append(far_own * far_own + turn[0])
    far_reach.append(far_own * far_reach[1] + turn[0] * far_own + turn[1])
    lists = [far_gain[i] * far_chain[k] for k in range(5) for i in range(3)]
    squares_of = [far_gain[i] * far_gain[m] for i, m in PAIRS]
    lists += squares_of + [q * far_reach[n] for n in range(3) for q in squares_of]
    block = over_senders(lists)

    def squares(power, i, m):
        at = 15 + power * 6 + PAIRS.index((min(i, m), max(i, m)))
        return block[at : at + 1, :]

    found = solve(lambda k, i: block[3 * k + i : 3 * k + i + 1, :], squares)
    sent_total = [found[0][i] + found[1][i] + found[2][i] + found[3][i] + found[4][i] for i in range(3)]
    for k in range(4):
        z = sum(far_gain[i] * found[k][i] for i in range(3))
        for s in range(ST):
            b_out[s, k : k + 1, :] = z[s : s + 1, :]
    for i in range(3):
        moved = mine[i : i + 1, :] + mine[3 + i : 4 + i, :] - sent_total[i]
        for s in range(ST):
            b_out[s, 4 + i : 5 + i, :] = moved
    for s in range(ST):
        b_out[s, 7:8, :] = jnp.zeros((1, LANES), F32)
    start(3, lambda b: b_out.at[b // 8], b_in, -1)


    label = climb(climb(label_two))
    atom_bond = inverse[0:16, :].astype(I32)
    bond_at = jnp.maximum(atom_bond - 1, 0)
    atom_label = lookup([label[t : t + 1, :] for t in range(BT)], bond_at // LANES, bond_at % LANES)
    row16 = lax.broadcasted_iota(I32, (16, LANES), 0)
    atom_label = jnp.where(
        jnp.logical_and(atom_bond > 0, row16 < AT), atom_label, 0.0
    ).astype(I32)
    label = label.astype(I32)

    def labelled(tiles, which):
        at = jnp.maximum(which - 1, 0)
        return jnp.where(which > 0, lookup(tiles, at // LANES, at % LANES), 0.0)

    unit = jnp.where(is_halo, 1.0, 0.0)
    chain, reach = [right], [unit]
    for _ in range(3):
        nxt = couple([chain[-1], reach[-1]])
        chain.append(nxt[0])
        reach.append(nxt[1])
    chain.append(couple([chain[-1]])[0])
    base = chain[0] + chain[1] + chain[2] + chain[3] + chain[4]
    grown = [reach[0]]
    for m in range(1, 4):
        grown.append(grown[-1] + reach[m])
    to_atoms([v * g for v in [base] + grown for g in gain])
    moves = []
    for n in range(15):
        moves.append(difference(n))
    for n in range(15):
        for j in range(AT):
            gathered[n, j : j + 1, :] = sums[j, n : n + 1, :]
        gathered[n, AT:16, :] = jnp.zeros((16 - AT, LANES), F32)

    all_of(3, b_in).wait_recv()
    back = merge(b_in, 8)

    def kind_rows(tiles, k):
        return [tiles[s][k : k + 1, :] for s in range(ST)]

    z = [labelled(kind_rows(back, k), label) for k in range(4)]
    far_pos = [labelled(kind_rows(back, 4 + i), label) for i in range(3)]
    sol_one = base
    for j in range(4):
        sol_one = sol_one + z[j] * grown[3 - j]
    current = None
    for i in range(3):
        ahead = head_new[i] - jnp.where(is_halo, far_pos[i], tail_new[i])
        step = moves[i]
        for j in range(4):
            step = step + z[j] * moves[3 * (1 + 3 - j) + i]
        stretch = ahead - step
        current = stretch * stretch if current is None else current + stretch * stretch
    target = jnp.sqrt(jnp.maximum(2.0 * length * length - current, 0.5 * length * length))
    chain_two = [scale * (length - target)]
    for _ in range(2):
        chain_two.append(couple([chain_two[-1]])[0])
    tree_sums = times_ones(
        [unit * v for v in chain_two] + [reach[1] * chain_two[2], reach[2] * chain_two[2]],
        trees_of[...],
    )
    for s in range(ST):
        c_out[s] = tree_sums[0:8, s * LANES : (s + 1) * LANES]
    start(4, lambda b: c_out.at[b // 8], c_in, 1)
    for _ in range(2):
        chain_two.append(couple([chain_two[-1]])[0])

    base_two = chain_two[0] + chain_two[1] + chain_two[2] + chain_two[3] + chain_two[4]
    to_atoms([base_two * g for g in gain])
    mass_atoms = jnp.concatenate(
        [table[j, 6:7, :] for j in range(AT)] + [jnp.zeros((16 - AT, LANES), F32)], axis=0
    )
    still = []
    for i in range(3):
        spread_base = jnp.concatenate(
            [gathered[i, j : j + 1, :] + sums[j, i : i + 1, :] for j in range(AT)]
            + [jnp.zeros((16 - AT, LANES), F32)],
            axis=0,
        )
        start_pos = jnp.concatenate(
            [table[j, i : i + 1, :] + table[j, 3 + i : 4 + i, :] for j in range(AT)]
            + [jnp.zeros((16 - AT, LANES), F32)],
            axis=0,
        )
        still.append(start_pos - mass_atoms * spread_base)
    trees = [[mass_atoms * gathered[3 * (1 + n) + i] for i in range(3)] for n in range(4)]
    number16 = row16 * LANES + lax.broadcasted_iota(I32, (16, LANES), 1)
    which = jnp.zeros((16, LANES), I32)
    for e in range(SEND):
        which = jnp.where(number16 == sent8[0:1, e : e + 1], e + 1, which)

    all_of(4, c_in).wait_recv()
    far_two = by_kind(merge(c_in, 8), 5)
    block_two = over_senders([far_gain[i] * far_two[k] for k in range(5) for i in range(3)])
    found_two = solve(lambda k, i: block_two[3 * k + i : 3 * k + i + 1, :], squares)
    for k in range(4):
        z_two = sum(far_gain[i] * found_two[k][i] for i in range(3))
        for s in range(ST):
            d_out[s, k : k + 1, :] = z_two[s : s + 1, :]
    start(5, lambda b: d_out.at[b // 8], d_in, -1)

    for i in range(3):
        total = sent_total[i]
        for k in range(5):
            total = total + found_two[k][i]
        own_move = take(jnp.broadcast_to(total, (16, LANES)), jnp.maximum(which - 1, 0))
        still[i] = still[i] - jnp.where(which > 0, own_move, 0.0)

    all_of(5, d_in).wait_recv()
    last = merge(d_in, 4)
    result = sol_one + base_two
    for j in range(4):
        result = result + labelled(kind_rows(last, j), label) * grown[3 - j]
    for t in range(BT):
        mult_ref[:, t * LANES : (t + 1) * LANES] = result[t : t + 1, :]
    both = [[back[s][k : k + 1, :] + last[s][k : k + 1, :] for s in range(ST)] for k in range(4)]
    for j in range(4):
        z_atom = labelled(both[j], atom_label)
        for i in range(3):
            still[i] = still[i] - z_atom * trees[3 - j][i]
    for i in range(3):
        for j in range(AT):
            at = i * ATOMS + j * LANES
            new_ref[:, at : at + LANES] = still[i][j : j + 1, :]

    for stage, target in ((0, r0_in), (1, a_in), (3, b_in), (4, c_in), (5, d_in)):
        all_of(stage, target).wait_send()


def write_out(new_ref, mult_ref, new_out, mult_out):
    new_out[...] = new_ref[...]
    mult_out[...] = mult_ref[...]


def solution(mesh):
    sizes = tuple(mesh.shape[n] for n in ("gx", "gy", "gz"))

    def per_device(old_pos, displacement, inv_mass, bond_head, bond_tail, send_list):
        near = len(BLOCKS)
        vmem = pl.BlockSpec(memory_space=pltpu.VMEM)
        new_pos, multipliers = pl.pallas_call(
            functools.partial(kernel, sizes),
            out_shape=(pltpu.VMEM((1, 3 * ATOMS), F32), pltpu.VMEM((1, BONDS), F32)),
            in_specs=[pl.BlockSpec(memory_space=pl.ANY)] * 6,
            out_specs=(vmem, vmem),
            scratch_shapes=[
                pltpu.VMEM((3, 1, ATOMS), F32),
                pltpu.VMEM((3, 1, ATOMS), F32),
                pltpu.VMEM((1, ATOMS), F32),
                pltpu.VMEM((1, BONDS), I32),
                pltpu.VMEM((1, BONDS), I32),
                pltpu.VMEM((1, SEND), I32),
                pltpu.SemaphoreType.DMA((6,)),
                pltpu.VMEM((AT, 8, LANES), F32),
                pltpu.VMEM((2, 8, LANES), I32),
                pltpu.VMEM((7, BONDS, LANES), F32),
                pltpu.VMEM((BONDS, ATOMS), jnp.bfloat16),
                pltpu.VMEM((BONDS, ST * LANES), jnp.bfloat16),
                pltpu.VMEM((BONDS, BONDS), F32),
                pltpu.VMEM((AT + ST, 8, LANES), F32),
                pltpu.VMEM((AT + ST, LANES), F32),
                pltpu.VMEM((2, 8, LANES), F32),
                pltpu.VMEM((5, 8, LANES), F32),
                pltpu.VMEM((AT, 16, LANES), F32),
                pltpu.VMEM((8, 40, LANES), F32),
                pltpu.VMEM((15, 16, LANES), F32),
                pltpu.VMEM((8, LANES), F32),
                pltpu.VMEM((near, 8, LANES), F32),
                pltpu.VMEM((ST, 8, LANES), F32),
                pltpu.VMEM((ST, 8, LANES), F32),
                pltpu.VMEM((ST, 4, LANES), F32),
                pltpu.VMEM((near, 8, LANES), F32),
                pltpu.VMEM((near, 8, LANES), F32),
                pltpu.VMEM((near, 8, LANES), F32),
                pltpu.VMEM((near, 8, LANES), F32),
                pltpu.VMEM((near, 4, LANES), F32),
                pltpu.SemaphoreType.DMA((6,)),
                pltpu.SemaphoreType.DMA((6,)),
            ],
            compiler_params=pltpu.CompilerParams(collective_id=0, has_side_effects=True),
        )(
            old_pos.reshape(3, 1, ATOMS),
            displacement.reshape(3, 1, ATOMS),
            inv_mass.reshape(1, ATOMS),
            bond_head.reshape(1, BONDS),
            bond_tail.reshape(1, BONDS),
            send_list.reshape(1, SEND),
        )
        new_pos, multipliers = pl.pallas_call(
            write_out,
            out_shape=(
                jax.ShapeDtypeStruct((1, 3 * ATOMS), F32),
                jax.ShapeDtypeStruct((1, BONDS), F32),
            ),
            in_specs=[vmem] * 2,
            out_specs=(vmem, vmem),
        )(
            pltpu.with_memory_space_constraint(new_pos, pltpu.VMEM),
            pltpu.with_memory_space_constraint(multipliers, pltpu.VMEM),
        )
        return new_pos.reshape(old_pos.shape), multipliers.reshape(bond_head.shape)

    return jax.shard_map(
        per_device,
        mesh=mesh,
        in_specs=(
            P(None, "gx", "gy", "gz", None),
            P(None, "gx", "gy", "gz", None),
            P("gx", "gy", "gz", None),
            P("gx", "gy", "gz", None),
            P("gx", "gy", "gz", None),
            P("gx", "gy", "gz", None),
        ),
        out_specs=(P(None, "gx", "gy", "gz", None), P("gx", "gy", "gz", None)),
        check_vma=False,
    )
```

```python
import functools

import jax
import jax.numpy as jnp
from jax import lax
from jax.experimental import pallas as pl
from jax.experimental.pallas import tpu as pltpu
from jax.sharding import PartitionSpec as P

MESH = pl.DeviceIdType.MESH
ATOMS = 1536
BONDS = 1024
SEND = 16
LANES = 128
AT = ATOMS // LANES
BT = BONDS // LANES
ST = 4
BLOCKS = [b for b in range(27) if b != 13]
ROW_OF = {b: n for n, b in enumerate(BLOCKS)}
F32 = jnp.float32
I32 = jnp.int32
PAIRS = [(0, 0), (0, 1), (0, 2), (1, 1), (1, 2), (2, 2)]


def take(rows, lane):
    numbers = lax.GatherDimensionNumbers(
        offset_dims=(),
        collapsed_slice_dims=(1,),
        start_index_map=(1,),
        operand_batching_dims=(0,),
        start_indices_batching_dims=(0,),
    )
    return lax.gather(
        rows, lane[..., None], numbers, (1, 1), mode=lax.GatherScatterMode.PROMISE_IN_BOUNDS
    )


def lookup(tiles, tile, lane):
    out = jnp.zeros(lane.shape, F32)
    for j, row in enumerate(tiles):
        out = jnp.where(tile == j, take(jnp.broadcast_to(row, lane.shape), lane), out)
    return out


def kernel(
    sizes,
    old_hbm,
    move_hbm,
    mass_hbm,
    head_hbm,
    tail_hbm,
    send_hbm,
    new_ref,
    mult_ref,
    old_ref,
    move_ref,
    mass_ref,
    head_ref,
    tail_ref,
    send_ref,
    load_sem,
    table,
    idx,
    cols,
    incidence,
    trees_of,
    coupling,
    found_by,
    inverse,
    vec,
    rows,
    sums,
    kinds,
    gathered,
    r0_out,
    a_out,
    a2_out,
    b_out,
    c_out,
    d_out,
    r0_in,
    a_in,
    a2_in,
    b_in,
    c_in,
    d_in,
    send_sem,
    recv_sem,
):
    loads = [
        pltpu.make_async_copy(source, target, load_sem.at[n])
        for n, (source, target) in enumerate(
            (
                (send_hbm, send_ref),
                (old_hbm, old_ref),
                (move_hbm, move_ref),
                (mass_hbm, mass_ref),
                (head_hbm, head_ref),
                (tail_hbm, tail_ref),
            )
        )
    ]
    for load in loads:
        load.start()
    names = ("gx", "gy", "gz")
    me = [lax.axis_index(n) for n in names]

    def device(block, sign):
        offs = (block // 9 - 1, block // 3 % 3 - 1, block % 3 - 1)
        return tuple(lax.rem(m + sign * o + n, n) for m, o, n in zip(me, offs, sizes))

    barrier = pltpu.get_barrier_semaphore()
    for b in BLOCKS:
        pl.semaphore_signal(barrier, inc=1, device_id=device(b, 1), device_id_type=MESH)

    def start(stage, source, target, sign):
        for b in BLOCKS:
            pltpu.make_async_remote_copy(
                src_ref=source(b),
                dst_ref=target.at[ROW_OF[b]],
                send_sem=send_sem.at[stage],
                recv_sem=recv_sem.at[stage],
                device_id=device(b, sign),
                device_id_type=MESH,
            ).start()

    def all_of(stage, target):
        return pltpu.make_async_remote_copy(
            src_ref=target,
            dst_ref=target,
            send_sem=send_sem.at[stage],
            recv_sem=recv_sem.at[stage],
            device_id=device(0, 1),
            device_id_type=MESH,
        )

    lane8 = lax.broadcasted_iota(I32, (8, LANES), 1)
    group8 = lane8 // SEND
    sub128 = lax.broadcasted_iota(I32, (LANES, LANES), 0)
    lane128 = lax.broadcasted_iota(I32, (LANES, LANES), 1)
    eye = sub128 == lane128

    for load in loads:
        load.wait()
    for j in range(AT):
        cut = pl.ds(j * LANES, LANES)
        for i in range(3):
            table[j, i : i + 1, :] = old_ref[i, :, cut]
            table[j, 3 + i : 4 + i, :] = move_ref[i, :, cut]
        table[j, 6:7, :] = mass_ref[:, cut]
        table[j, 7:8, :] = jnp.zeros((1, LANES), F32)
    sent8 = jnp.broadcast_to(
        jnp.concatenate([send_ref[...]] * (LANES // SEND), axis=1), (8, LANES)
    )
    mine = jnp.zeros((8, LANES), F32)
    for j in range(AT):
        mine = jnp.where(sent8 // LANES == j, take(table[j], sent8 % LANES), mine)
    r0_out[...] = mine

    for t in range(BT):
        cut = pl.ds(t * LANES, LANES)
        idx[0, t : t + 1, :] = head_ref[:, cut]
        idx[1, t : t + 1, :] = tail_ref[:, cut]
    head = idx[0]
    tail = idx[1]
    is_halo = tail >= ATOMS
    slot = jnp.where(is_halo, tail - ATOMS, 0)
    near = jnp.where(is_halo, 0, tail)

    def at_ends(row):
        tiles = [row(j) for j in range(AT)]
        return (
            lookup(tiles, head // LANES, head % LANES),
            lookup(tiles, near // LANES, near % LANES),
        )

    ends = [at_ends(lambda j, k=k: table[j, k : k + 1, :]) for k in range(7)]
    head_mass = ends[6][0]
    near_mass = jnp.where(is_halo, 0.0, ends[6][1])
    head_data = [e[0] for e in ends]
    head_new = [head_data[i] + head_data[3 + i] for i in range(3)]

    def to_cols(k, value):
        for t in range(BT):
            col = jnp.sum(jnp.where(eye, value[t : t + 1, :], 0.0), axis=1, keepdims=True)
            cols[k, t * LANES : (t + 1) * LANES, :] = jnp.broadcast_to(col, (LANES, LANES))

    to_cols(0, head.astype(F32))
    to_cols(1, tail.astype(F32))

    def geometry(ahead, behind, mass, ahead_new, behind_new):
        bond = [p - q for p, q in zip(ahead, behind)]
        length = jnp.maximum(
            jnp.sqrt(bond[0] * bond[0] + bond[1] * bond[1] + bond[2] * bond[2]), 0.5
        )
        direction = [b / length for b in bond]
        scale = 1.0 / jnp.sqrt(mass)
        shift = [p - q for p, q in zip(ahead_new, behind_new)]
        right = scale * (
            direction[0] * shift[0] + direction[1] * shift[1] + direction[2] * shift[2] - length
        )
        return length, scale, [scale * d for d in direction], right

    near_data = [e[1] for e in ends]
    _, _, tree_gain, tree_right = geometry(
        head_data[0:3],
        near_data[0:3],
        head_mass + near_data[6],
        head_new,
        [near_data[i] + near_data[3 + i] for i in range(3)],
    )
    tree_gain = [jnp.where(is_halo, 0.0, g) for g in tree_gain]
    tree_right = jnp.where(is_halo, 0.0, tree_right)

    found_by[...] = jnp.zeros(found_by.shape, F32)
    kinds[...] = jnp.zeros(kinds.shape, F32)

    def incidence_rows(t, carry):
        here = pl.ds(pl.multiple_of(t * LANES, LANES), LANES)
        heads = cols[0, here, :]
        tails = cols[1, here, :]
        number = (sub128 + (t * LANES + 1)).astype(F32)
        cuts = [slice(8 * r, 8 * r + 8) for r in range(LANES // 8)]
        for j in range(AT + ST):
            atom = (lane8 + j * LANES).astype(F32)
            number_of = found_by[j]
            parts = []
            for cut in cuts:
                if j < AT:
                    found = heads[cut] == atom
                    parts.append(
                        jnp.where(found, 1.0, jnp.where(tails[cut] == atom, -1.0, 0.0))
                    )
                else:
                    found = tails[cut] == atom
                number_of = jnp.where(found, number[cut], number_of)
            found_by[j] = number_of
            if j < AT:
                incidence[here, j * LANES : (j + 1) * LANES] = jnp.concatenate(
                    parts, axis=0
                ).astype(jnp.bfloat16)
        return carry

    lax.fori_loop(0, 2, incidence_rows, 0)
    pl.semaphore_wait(barrier, len(BLOCKS))
    start(0, lambda b: r0_out, r0_in, -1)
    lax.fori_loop(2, BT, incidence_rows, 0)
    for j in range(AT + ST):
        inverse[j : j + 1, :] = jnp.sum(found_by[j], axis=0, keepdims=True)

    parent = lookup(
        [inverse[j : j + 1, :] for j in range(AT)], near // LANES, near % LANES
    ).astype(I32)
    has_parent = jnp.logical_and(parent > 0, jnp.logical_not(is_halo))
    parent = jnp.maximum(parent - 1, 0)
    root = jnp.where(is_halo, slot + 1, 0).astype(F32)

    def climb(label):
        above = lookup([label[t : t + 1, :] for t in range(BT)], parent // LANES, parent % LANES)
        return jnp.where(has_parent, above, root)

    def put_kinds(values):
        for k, value in enumerate(values):
            for t in range(BT):
                kinds[t, k : k + 1, :] = value[t : t + 1, :]

    def times_ones(values, matrix):
        height = (len(values) + 15) // 16 * 16
        put_kinds(values)
        full = jnp.concatenate([kinds[t, :height, :] for t in range(BT)], axis=1)
        high = full.astype(jnp.bfloat16)
        rest = full - high.astype(F32)
        mid = rest.astype(jnp.bfloat16)
        low = (rest - mid.astype(F32)).astype(jnp.bfloat16)
        parts = jnp.concatenate([high, mid, low], axis=0)
        product = jnp.dot(parts, matrix, preferred_element_type=F32)
        return product[:height] + (product[height : 2 * height] + product[2 * height :])

    def to_atoms(weighted):
        total = times_ones(weighted, incidence[...])
        height = (len(weighted) + 7) // 8 * 8
        for j in range(AT):
            sums[j, :height, :] = total[:height, j * LANES : (j + 1) * LANES]

    def difference(n):
        at_head, at_near = at_ends(lambda j: sums[j, n : n + 1, :])
        return head_mass * at_head - near_mass * at_near

    label_one = climb(root)
    child = jnp.logical_and(label_one > 0.0, jnp.logical_not(is_halo))
    label_two = climb(label_one)
    start_of = [jnp.where(child, g, 0.0) for g in tree_gain]
    to_atoms(
        [tree_right * g for g in tree_gain]
        + [start_of[i] * tree_gain[m] for i, m in PAIRS]
    )
    diffs = [difference(n) for n in range(9)]
    tree_next = tree_right - sum(tree_gain[i] * diffs[i] for i in range(3))
    start_next = []
    for i in range(3):
        start_next.append(
            start_of[i]
            - sum(
                tree_gain[m] * diffs[3 + PAIRS.index((min(i, m), max(i, m)))] for m in range(3)
            )
        )
    label = climb(climb(label_two))
    to_cols(7, label)
    for s in range(ST):
        number = (lane128[0:1] + (s * LANES + 1)).astype(F32)
        trees_of[:, s * LANES : (s + 1) * LANES] = jnp.where(cols[7] == number, 1.0, 0.0).astype(
            jnp.bfloat16
        )
    tree_sums = times_ones(
        [start_of[i] * start_of[m] for i, m in PAIRS]
        + [start_of[i] * start_next[m] for i, m in PAIRS]
        + [start_next[i] * start_next[m] for i, m in PAIRS]
        + [y * tree_right for y in start_of]
        + [y * tree_next for y in start_of]
        + [y * tree_next for y in start_next],
        trees_of[...],
    )
    slots = inverse[AT : AT + ST, :].astype(I32)
    slot_bond = jnp.maximum(slots - 1, 0)
    slot_head = lookup(
        [head[t : t + 1, :].astype(F32) for t in range(BT)],
        slot_bond // LANES,
        slot_bond % LANES,
    ).astype(I32)
    for s in range(ST):
        at = jnp.broadcast_to(slot_head[s : s + 1, :], (8, LANES))
        used = jnp.broadcast_to(slots[s : s + 1, :], (8, LANES)) > 0
        atoms = jnp.zeros((8, LANES), F32)
        for j in range(AT):
            atoms = jnp.where(at // LANES == j, take(table[j], at % LANES), atoms)
        groups = [tree_sums[8 * n : 8 * n + 8, s * LANES : (s + 1) * LANES] for n in range(4)]
        groups.append(jnp.where(used, atoms, 0.0))
        turned = [pltpu.roll(g, SEND * n, axis=1) if n else g for n, g in enumerate(groups)]
        for b in BLOCKS:
            if b // 8 == s:
                out = turned[0]
                for n in range(1, len(turned)):
                    out = jnp.where(group8 == (b + n) % 8, turned[n], out)
                a_out[ROW_OF[b]] = out
    start(1, lambda b: a_out.at[ROW_OF[b]], a_in, 1)
    to_atoms([tree_next * g for g in tree_gain])
    diffs = [difference(n) for n in range(3)]
    tree_last = tree_next - sum(tree_gain[i] * diffs[i] for i in range(3))
    tree_sums = times_ones([y * tree_last for y in start_next], trees_of[...])
    for s in range(ST):
        a2_out[s] = tree_sums[0:4, s * LANES : (s + 1) * LANES]
    start(2, lambda b: a2_out.at[b // 8], a2_in, 1)

    def merge(source, width, turn=0):
        tiles = []
        for tile in range(ST):
            out = jnp.zeros((width, LANES), F32)
            for b in BLOCKS:
                if b // 8 == tile:
                    out = jnp.where(group8[:width] == (b + turn) % 8, source[ROW_OF[b]], out)
            if turn:
                out = pltpu.roll(out, LANES - SEND * turn, axis=1)
            tiles.append(out)
        return tiles

    to_cols(2, head_mass)
    to_cols(3, near_mass)
    rows[0] = head.astype(F32)
    rows[1] = tail.astype(F32)
    all_of(0, r0_in).wait_recv()
    halo = merge(r0_in, 8)
    slot_tile, slot_lane = slot // LANES, slot % LANES
    tail_data = []
    for k in range(7):
        far = lookup([halo[s][k : k + 1, :] for s in range(ST)], slot_tile, slot_lane)
        tail_data.append(jnp.where(is_halo, far, near_data[k]))
    tail_new = [tail_data[i] + tail_data[3 + i] for i in range(3)]
    length, scale, gain, right = geometry(
        head_data[0:3], tail_data[0:3], head_mass + tail_data[6], head_new, tail_new
    )
    own = 1.0 - head_mass * (gain[0] * gain[0] + gain[1] * gain[1] + gain[2] * gain[2])
    for i in range(3):
        to_cols(4 + i, gain[i])
    for i in range(3):
        rows[2 + i] = gain[i]

    def coupling_rows(t, carry):
        for part in range(2):
            here = pl.ds(pl.multiple_of(t * 64 + part * 32, 32), 32)
            heads, tails = cols[0, here, :], cols[1, here, :]
            masses, near_masses = cols[2, here, :], cols[3, here, :]
            minus_near = -near_masses
            gains = [cols[4 + i, here, :] for i in range(3)]
            for u in range(BT):
                head_row, tail_row = rows[0, u : u + 1, :], rows[1, u : u + 1, :]
                shared = jnp.where(
                    tails == head_row, minus_near, jnp.where(tails == tail_row, near_masses, 0.0)
                ) - jnp.where(heads == tail_row, masses, 0.0)
                dots = (
                    gains[0] * rows[2, u : u + 1, :]
                    + gains[1] * rows[3, u : u + 1, :]
                    + gains[2] * rows[4, u : u + 1, :]
                )
                coupling[here, u * LANES : (u + 1) * LANES] = shared * dots
        return carry

    lax.fori_loop(0, BONDS // 64, coupling_rows, 0)

    def couple(values):
        for n, value in enumerate(values):
            vec[n] = value
        outs = [[] for _ in values]
        for t in range(BT):
            for n in range(len(values)):
                total = None
                for u in range(BT):
                    part = (
                        coupling[t * LANES : (t + 1) * LANES, u * LANES : (u + 1) * LANES]
                        * vec[n, u : u + 1, :]
                    )
                    total = part if total is None else total + part
                col = jnp.sum(total, axis=1, keepdims=True)
                outs[n].append(jnp.sum(jnp.where(eye, col, 0.0), axis=0, keepdims=True))
        return [own * v - jnp.concatenate(o, axis=0) for v, o in zip(values, outs)]

    def by_kind(tiles, count):
        for s in range(ST):
            kinds[s, 0 : tiles[s].shape[0], :] = tiles[s]
        return [
            jnp.concatenate([kinds[s, k : k + 1, :] for s in range(ST)], axis=0)
            for k in range(count)
        ]

    def over_senders(values):
        lines = [jnp.sum(v, axis=0, keepdims=True) for v in values]
        lines += [jnp.zeros((1, LANES), F32)] * (-len(lines) % 8)
        block = jnp.concatenate(lines, axis=0)
        turned = [pltpu.roll(block, SEND * n, axis=1) for n in range(1, LANES // SEND)]
        return ((block + turned[0]) + (turned[1] + turned[2])) + (
            (turned[3] + turned[4]) + (turned[5] + turned[6])
        )

    own_mass = mine[6:7, :]

    def solve(sums_of, squares, found, count):
        for k in range(len(found), count):
            now = []
            for i in range(3):
                total = sums_of(k, i)
                for j in range(k):
                    for m in range(3):
                        total = total + squares(k - 1 - j, i, m) * found[j][m]
                now.append(-own_mass * total)
            found.append(now)
        return found

    all_of(1, a_in).wait_recv()
    far = []
    for n in range(5):
        far += by_kind(merge(a_in, 8, n), 8)
    far_head, far_mass = far[32:38], far[38]
    far_new = [far_head[i] + far_head[3 + i] for i in range(3)]
    used = far_mass > 0.0
    far_length, far_scale, far_gain, far_right = geometry(
        far_head[0:3],
        [mine[i : i + 1, :] for i in range(3)],
        far_mass + own_mass,
        far_new,
        [mine[i : i + 1, :] + mine[3 + i : 4 + i, :] for i in range(3)],
    )
    far_gain = [jnp.where(used, g, 0.0) for g in far_gain]
    far_right = jnp.where(used, far_right, 0.0)
    pull = [far_mass * g for g in far_gain]
    far_own = 1.0 - (pull[0] * far_gain[0] + pull[1] * far_gain[1] + pull[2] * far_gain[2])
    turn = []
    for power in range(3):
        form = far[6 * power : 6 * power + 6]
        turn.append(
            sum(
                pull[i] * sum(pull[m] * form[PAIRS.index((min(i, m), max(i, m)))] for m in range(3))
                for i in range(3)
            )
        )
    feed = [sum(pull[i] * far[18 + 3 * k + i] for i in range(3)) for k in range(3)]
    far_chain = [far_right]

    def next_chain():
        k = len(far_chain) - 1
        value = far_own * far_chain[k] + feed[k]
        for j in range(k):
            value = value + turn[k - 1 - j] * far_chain[j]
        far_chain.append(value)

    for _ in range(3):
        next_chain()
    far_reach = [far_own]
    far_reach.append(far_own * far_own + turn[0])
    far_reach.append(far_own * far_reach[1] + turn[0] * far_own + turn[1])
    lists = [far_gain[i] * far_chain[k] for k in range(4) for i in range(3)]
    squares_of = [far_gain[i] * far_gain[m] for i, m in PAIRS]
    lists += squares_of + [q * far_reach[n] for n in range(3) for q in squares_of]
    block = over_senders(lists)

    def squares(power, i, m):
        at = 12 + power * 6 + PAIRS.index((min(i, m), max(i, m)))
        return block[at : at + 1, :]

    found = solve(lambda k, i: block[3 * k + i : 3 * k + i + 1, :], squares, [], 4)
    for k in range(4):
        z = sum(far_gain[i] * found[k][i] for i in range(3))
        for s in range(ST):
            b_out[s, k : k + 1, :] = z[s : s + 1, :]
    start(3, lambda b: b_out.at[b // 8], b_in, -1)


    atom_bond = inverse[0:16, :].astype(I32)
    bond_at = jnp.maximum(atom_bond - 1, 0)
    atom_label = lookup([label[t : t + 1, :] for t in range(BT)], bond_at // LANES, bond_at % LANES)
    row16 = lax.broadcasted_iota(I32, (16, LANES), 0)
    atom_label = jnp.where(
        jnp.logical_and(atom_bond > 0, row16 < AT), atom_label, 0.0
    ).astype(I32)
    label = label.astype(I32)

    def labelled(tiles, which):
        at = jnp.maximum(which - 1, 0)
        return jnp.where(which > 0, lookup(tiles, at // LANES, at % LANES), 0.0)

    unit = jnp.where(is_halo, 1.0, 0.0)
    chain, reach = [right], [unit]
    for _ in range(4):
        nxt = couple([chain[-1], reach[-1]])
        chain.append(nxt[0])
        reach.append(nxt[1])
    base = chain[0] + chain[1] + chain[2] + chain[3] + chain[4]
    grown = [reach[0]]
    for m in range(1, 5):
        grown.append(grown[-1] + reach[m])
    to_atoms([v * g for v in [base] + grown[:4] for g in gain])
    moves = []
    for n in range(15):
        moves.append(difference(n))
    for n in range(15):
        for j in range(AT):
            gathered[n, j : j + 1, :] = sums[j, n : n + 1, :]
        gathered[n, AT:16, :] = jnp.zeros((16 - AT, LANES), F32)

    all_of(3, b_in).wait_recv()
    back = merge(b_in, 4)

    def kind_rows(tiles, k):
        return [tiles[s][k : k + 1, :] for s in range(ST)]

    z = [labelled(kind_rows(back, k), label) for k in range(4)]
    sol_one = base
    for j in range(4):
        sol_one = sol_one + z[j] * grown[3 - j]
    current = None
    moved = []
    for i in range(3):
        ahead = head_new[i] - jnp.where(is_halo, 0.0, tail_new[i])
        step = moves[i]
        for j in range(4):
            step = step + z[j] * moves[3 * (1 + 3 - j) + i]
        stretch = ahead - step
        moved.append(stretch)
        current = stretch * stretch if current is None else current + stretch * stretch

    def second_right(scale, length, current):
        target = jnp.sqrt(jnp.maximum(2.0 * length * length - current, 0.5 * length * length))
        return scale * (length - target)

    chain_two = [jnp.where(is_halo, 0.0, second_right(scale, length, current))]
    tree_sums = times_ones(
        [reach[k] * chain_two[0] for k in range(1, 5)] + [unit * m for m in moved],
        trees_of[...],
    )
    for s in range(ST):
        c_out[s] = tree_sums[0:8, s * LANES : (s + 1) * LANES]
    start(4, lambda b: c_out.at[b // 8], c_in, 1)
    for _ in range(4):
        chain_two.append(couple([chain_two[-1]])[0])

    base_two = chain_two[0] + chain_two[1] + chain_two[2] + chain_two[3] + chain_two[4]
    to_atoms([v * g for v in (base_two, grown[4]) for g in gain])
    mass_atoms = jnp.concatenate(
        [table[j, 6:7, :] for j in range(AT)] + [jnp.zeros((16 - AT, LANES), F32)], axis=0
    )
    still = []
    for i in range(3):
        spread_base = jnp.concatenate(
            [gathered[i, j : j + 1, :] + sums[j, i : i + 1, :] for j in range(AT)]
            + [jnp.zeros((16 - AT, LANES), F32)],
            axis=0,
        )
        start_pos = jnp.concatenate(
            [table[j, i : i + 1, :] + table[j, 3 + i : 4 + i, :] for j in range(AT)]
            + [jnp.zeros((16 - AT, LANES), F32)],
            axis=0,
        )
        still.append(start_pos - mass_atoms * spread_base)
    trees = [[mass_atoms * gathered[3 * (1 + n) + i] for i in range(3)] for n in range(4)]
    no_atoms = jnp.zeros((16 - AT, LANES), F32)
    trees.append(
        [
            mass_atoms
            * jnp.concatenate([sums[j, 3 + i : 4 + i, :] for j in range(AT)] + [no_atoms], axis=0)
            for i in range(3)
        ]
    )
    all_of(2, a2_in).wait_recv()
    late = by_kind(merge(a2_in, 4), 3)
    feed.append(sum(pull[i] * late[i] for i in range(3)))
    next_chain()
    far_reach.append(
        far_own * far_reach[2] + turn[0] * far_reach[1] + turn[1] * far_own + turn[2]
    )
    last_sum = over_senders([far_gain[i] * far_chain[4] for i in range(3)])
    solve(lambda k, i: last_sum[i : i + 1, :], squares, found, 5)
    sent_total = [
        found[0][i] + found[1][i] + found[2][i] + found[3][i] + found[4][i] for i in range(3)
    ]
    sent_moved = [mine[i : i + 1, :] + mine[3 + i : 4 + i, :] - sent_total[i] for i in range(3)]
    number16 = row16 * LANES + lax.broadcasted_iota(I32, (16, LANES), 1)
    which = jnp.zeros((16, LANES), I32)
    for e in range(SEND):
        which = jnp.where(number16 == sent8[0:1, e : e + 1], e + 1, which)

    all_of(4, c_in).wait_recv()
    far_two = by_kind(merge(c_in, 8), 7)
    apart = [far_two[4 + i] - sent_moved[i] for i in range(3)]
    far_right_two = second_right(
        far_scale, far_length, apart[0] * apart[0] + apart[1] * apart[1] + apart[2] * apart[2]
    )
    far_right_two = jnp.where(used, far_right_two, 0.0)
    far_chain_two = [far_right_two]
    for k in range(4):
        far_chain_two.append(far_two[k] + far_reach[k] * far_right_two)
    block_two = over_senders([far_gain[i] * far_chain_two[k] for k in range(5) for i in range(3)])
    found_two = solve(lambda k, i: block_two[3 * k + i : 3 * k + i + 1, :], squares, [], 5)
    for k in range(4):
        z_two = sum(far_gain[i] * found_two[k][i] for i in range(3))
        for s in range(ST):
            d_out[s, k : k + 1, :] = z_two[s : s + 1, :]
    for s in range(ST):
        d_out[s, 4:5, :] = far_right_two[s : s + 1, :]
        d_out[s, 5:8, :] = jnp.zeros((3, LANES), F32)
    start(5, lambda b: d_out.at[b // 8], d_in, -1)

    for i in range(3):
        total = sent_total[i]
        for k in range(5):
            total = total + found_two[k][i]
        own_move = take(jnp.broadcast_to(total, (16, LANES)), jnp.maximum(which - 1, 0))
        still[i] = still[i] - jnp.where(which > 0, own_move, 0.0)

    all_of(5, d_in).wait_recv()
    last = merge(d_in, 8)
    result = sol_one + base_two
    for j in range(5):
        result = result + labelled(kind_rows(last, j), label) * grown[3 - j if j < 4 else 4]
    for t in range(BT):
        mult_ref[:, t * LANES : (t + 1) * LANES] = result[t : t + 1, :]
    both = [[back[s][k : k + 1, :] + last[s][k : k + 1, :] for s in range(ST)] for k in range(4)]
    both.append(kind_rows(last, 4))
    for j in range(5):
        z_atom = labelled(both[j], atom_label)
        for i in range(3):
            still[i] = still[i] - z_atom * trees[3 - j if j < 4 else 4][i]
    for i in range(3):
        for j in range(AT):
            at = i * ATOMS + j * LANES
            new_ref[:, at : at + LANES] = still[i][j : j + 1, :]

    for stage, target in ((0, r0_in), (1, a_in), (2, a2_in), (3, b_in), (4, c_in), (5, d_in)):
        all_of(stage, target).wait_send()


def write_out(new_ref, mult_ref, new_out, mult_out):
    new_out[...] = new_ref[...]
    mult_out[...] = mult_ref[...]


def solution(mesh):
    sizes = tuple(mesh.shape[n] for n in ("gx", "gy", "gz"))

    def per_device(old_pos, displacement, inv_mass, bond_head, bond_tail, send_list):
        near = len(BLOCKS)
        vmem = pl.BlockSpec(memory_space=pltpu.VMEM)
        new_pos, multipliers = pl.pallas_call(
            functools.partial(kernel, sizes),
            out_shape=(pltpu.VMEM((1, 3 * ATOMS), F32), pltpu.VMEM((1, BONDS), F32)),
            in_specs=[pl.BlockSpec(memory_space=pl.ANY)] * 6,
            out_specs=(vmem, vmem),
            scratch_shapes=[
                pltpu.VMEM((3, 1, ATOMS), F32),
                pltpu.VMEM((3, 1, ATOMS), F32),
                pltpu.VMEM((1, ATOMS), F32),
                pltpu.VMEM((1, BONDS), I32),
                pltpu.VMEM((1, BONDS), I32),
                pltpu.VMEM((1, SEND), I32),
                pltpu.SemaphoreType.DMA((6,)),
                pltpu.VMEM((AT, 8, LANES), F32),
                pltpu.VMEM((2, 8, LANES), I32),
                pltpu.VMEM((8, BONDS, LANES), F32),
                pltpu.VMEM((BONDS, ATOMS), jnp.bfloat16),
                pltpu.VMEM((BONDS, ST * LANES), jnp.bfloat16),
                pltpu.VMEM((BONDS, BONDS), F32),
                pltpu.VMEM((AT + ST, 8, LANES), F32),
                pltpu.VMEM((AT + ST, LANES), F32),
                pltpu.VMEM((2, 8, LANES), F32),
                pltpu.VMEM((5, 8, LANES), F32),
                pltpu.VMEM((AT, 16, LANES), F32),
                pltpu.VMEM((8, 40, LANES), F32),
                pltpu.VMEM((15, 16, LANES), F32),
                pltpu.VMEM((8, LANES), F32),
                pltpu.VMEM((near, 8, LANES), F32),
                pltpu.VMEM((ST, 4, LANES), F32),
                pltpu.VMEM((ST, 4, LANES), F32),
                pltpu.VMEM((ST, 8, LANES), F32),
                pltpu.VMEM((ST, 8, LANES), F32),
                pltpu.VMEM((near, 8, LANES), F32),
                pltpu.VMEM((near, 8, LANES), F32),
                pltpu.VMEM((near, 4, LANES), F32),
                pltpu.VMEM((near, 4, LANES), F32),
                pltpu.VMEM((near, 8, LANES), F32),
                pltpu.VMEM((near, 8, LANES), F32),
                pltpu.SemaphoreType.DMA((6,)),
                pltpu.SemaphoreType.DMA((6,)),
            ],
            compiler_params=pltpu.CompilerParams(collective_id=0, has_side_effects=True),
        )(
            old_pos.reshape(3, 1, ATOMS),
            displacement.reshape(3, 1, ATOMS),
            inv_mass.reshape(1, ATOMS),
            bond_head.reshape(1, BONDS),
            bond_tail.reshape(1, BONDS),
            send_list.reshape(1, SEND),
        )
        new_pos, multipliers = pl.pallas_call(
            write_out,
            out_shape=(
                jax.ShapeDtypeStruct((1, 3 * ATOMS), F32),
                jax.ShapeDtypeStruct((1, BONDS), F32),
            ),
            in_specs=[vmem] * 2,
            out_specs=(vmem, vmem),
        )(
            pltpu.with_memory_space_constraint(new_pos, pltpu.VMEM),
            pltpu.with_memory_space_constraint(multipliers, pltpu.VMEM),
        )
        return new_pos.reshape(old_pos.shape), multipliers.reshape(bond_head.shape)

    return jax.shard_map(
        per_device,
        mesh=mesh,
        in_specs=(
            P(None, "gx", "gy", "gz", None),
            P(None, "gx", "gy", "gz", None),
            P("gx", "gy", "gz", None),
            P("gx", "gy", "gz", None),
            P("gx", "gy", "gz", None),
            P("gx", "gy", "gz", None),
        ),
        out_specs=(P(None, "gx", "gy", "gz", None), P("gx", "gy", "gz", None)),
        check_vma=False,
    )
```

```python
import functools

import jax
import jax.numpy as jnp
from jax import lax
from jax.experimental import pallas as pl
from jax.experimental.pallas import tpu as pltpu
from jax.sharding import PartitionSpec as P

MESH = pl.DeviceIdType.MESH
ATOMS = 1536
BONDS = 1024
SEND = 16
LANES = 128
AT = ATOMS // LANES
BT = BONDS // LANES
ST = 4
BLOCKS = [b for b in range(27) if b != 13]
ROW_OF = {b: n for n, b in enumerate(BLOCKS)}
FAR_FIRST = sorted(BLOCKS, key=lambda b: (b // 9 == 1) + (b // 3 % 3 == 1) + (b % 3 == 1))
F32 = jnp.float32
I32 = jnp.int32
PAIRS = [(0, 0), (0, 1), (0, 2), (1, 1), (1, 2), (2, 2)]


def take(rows, lane):
    numbers = lax.GatherDimensionNumbers(
        offset_dims=(),
        collapsed_slice_dims=(1,),
        start_index_map=(1,),
        operand_batching_dims=(0,),
        start_indices_batching_dims=(0,),
    )
    return lax.gather(
        rows, lane[..., None], numbers, (1, 1), mode=lax.GatherScatterMode.PROMISE_IN_BOUNDS
    )


def lookup(tiles, tile, lane):
    out = jnp.zeros(lane.shape, F32)
    for j, row in enumerate(tiles):
        out = jnp.where(tile == j, take(jnp.broadcast_to(row, lane.shape), lane), out)
    return out


def kernel(
    sizes,
    old_hbm,
    move_hbm,
    mass_hbm,
    head_hbm,
    tail_hbm,
    send_hbm,
    new_ref,
    mult_ref,
    old_ref,
    move_ref,
    mass_ref,
    head_ref,
    tail_ref,
    send_ref,
    load_sem,
    table,
    idx,
    cols,
    incidence,
    trees_of,
    coupling,
    found_by,
    inverse,
    vec,
    rows,
    split,
    left_side,
    sums,
    kinds,
    gathered,
    r0_out,
    a_out,
    a2_out,
    b_out,
    c_out,
    d_out,
    r0_in,
    a_in,
    a2_in,
    b_in,
    c_in,
    d_in,
    send_sem,
    recv_sem,
):
    loads = [
        pltpu.make_async_copy(source, target, load_sem.at[n])
        for n, (source, target) in enumerate(
            (
                (send_hbm, send_ref),
                (old_hbm, old_ref),
                (move_hbm, move_ref),
                (mass_hbm, mass_ref),
                (head_hbm, head_ref),
                (tail_hbm, tail_ref),
            )
        )
    ]
    for load in loads:
        load.start()
    names = ("gx", "gy", "gz")
    me = [lax.axis_index(n) for n in names]

    near_by = [{o: lax.rem(m + o + n, n) if o else m for o in (-1, 0, 1)} for m, n in zip(me, sizes)]

    def device(block, sign):
        offs = (block // 9 - 1, block // 3 % 3 - 1, block % 3 - 1)
        return tuple(axis[sign * o] for axis, o in zip(near_by, offs))

    barrier = pltpu.get_barrier_semaphore()
    for b in BLOCKS:
        pl.semaphore_signal(barrier, inc=1, device_id=device(b, 1), device_id_type=MESH)

    def start(stage, source, target, sign):
        for b in FAR_FIRST:
            pltpu.make_async_remote_copy(
                src_ref=source(b),
                dst_ref=target.at[ROW_OF[b]],
                send_sem=send_sem.at[stage],
                recv_sem=recv_sem.at[stage],
                device_id=device(b, sign),
                device_id_type=MESH,
            ).start()

    def all_of(stage, target):
        return pltpu.make_async_remote_copy(
            src_ref=target,
            dst_ref=target,
            send_sem=send_sem.at[stage],
            recv_sem=recv_sem.at[stage],
            device_id=device(0, 1),
            device_id_type=MESH,
        )

    lane8 = lax.broadcasted_iota(I32, (8, LANES), 1)
    group8 = lane8 // SEND
    sub128 = lax.broadcasted_iota(I32, (LANES, LANES), 0)
    lane128 = lax.broadcasted_iota(I32, (LANES, LANES), 1)
    eye = sub128 == lane128

    for load in loads:
        load.wait()
    for j in range(AT):
        cut = pl.ds(j * LANES, LANES)
        for i in range(3):
            table[j, i : i + 1, :] = old_ref[i, :, cut]
            table[j, 3 + i : 4 + i, :] = move_ref[i, :, cut]
        table[j, 6:7, :] = mass_ref[:, cut]
        table[j, 7:8, :] = jnp.zeros((1, LANES), F32)
    sent8 = jnp.broadcast_to(
        jnp.concatenate([send_ref[...]] * (LANES // SEND), axis=1), (8, LANES)
    )
    mine = jnp.zeros((8, LANES), F32)
    for j in range(AT):
        mine = jnp.where(sent8 // LANES == j, take(table[j], sent8 % LANES), mine)
    r0_out[...] = mine

    for t in range(BT):
        cut = pl.ds(t * LANES, LANES)
        idx[0, t : t + 1, :] = head_ref[:, cut]
        idx[1, t : t + 1, :] = tail_ref[:, cut]
    head = idx[0]
    tail = idx[1]
    is_halo = tail >= ATOMS
    slot = jnp.where(is_halo, tail - ATOMS, 0)
    near = jnp.where(is_halo, 0, tail)

    def at_ends(row):
        lines = [row(j) for j in range(AT)]
        return (
            lookup(lines, head // LANES, head % LANES),
            lookup(lines, near // LANES, near % LANES),
        )

    ends = [at_ends(lambda j, k=k: table[j, k : k + 1, :]) for k in range(7)]
    head_mass = ends[6][0]
    near_mass = jnp.where(is_halo, 0.0, ends[6][1])
    head_data = [e[0] for e in ends]
    head_new = [head_data[i] + head_data[3 + i] for i in range(3)]

    def to_cols(k, value):
        for t in range(BT):
            col = jnp.sum(jnp.where(eye, value[t : t + 1, :], 0.0), axis=1, keepdims=True)
            cols[k, t * LANES : (t + 1) * LANES, :] = jnp.broadcast_to(col, (LANES, LANES))

    rows[0] = head.astype(F32)
    rows[1] = tail.astype(F32)
    both_ends = rows[0] * 2048.0 + rows[1]
    for t in range(BT):
        here = slice(t * LANES, (t + 1) * LANES)
        col = jnp.sum(jnp.where(eye, both_ends[t : t + 1, :], 0.0), axis=1, keepdims=True)
        col = jnp.broadcast_to(col, (LANES, LANES))
        heads = jnp.floor(col * (1.0 / 2048.0))
        for k, value in enumerate((heads, col - 2048.0 * heads)):
            cols[k, here, :] = value

    found_by[...] = jnp.zeros(found_by.shape, F32)
    kinds[...] = jnp.zeros(kinds.shape, F32)
    split[...] = jnp.zeros(split.shape, F32)
    half = jnp.bfloat16

    def incidence_rows(t, carry):
        here = pl.ds(pl.multiple_of(t * LANES, LANES), LANES)
        heads = cols[0, here, :]
        tails = cols[1, here, :]
        number = (sub128 + (t * LANES + 1)).astype(F32)
        cuts = [slice(8 * r, 8 * r + 8) for r in range(LANES // 8)]
        for j in range(AT + ST):
            atom = (lane8 + j * LANES).astype(F32)
            number_of = found_by[j]
            parts = []
            for cut in cuts:
                if j < AT:
                    found = heads[cut] == atom
                    parts.append(
                        jnp.where(found, 1.0, jnp.where(tails[cut] == atom, -1.0, 0.0))
                    )
                else:
                    found = tails[cut] == atom
                number_of = jnp.where(found, number[cut], number_of)
            found_by[j] = number_of
            if j < AT:
                incidence[here, j * LANES : (j + 1) * LANES] = jnp.concatenate(
                    parts, axis=0
                ).astype(half)
        return carry

    lax.fori_loop(0, BT, incidence_rows, 0)
    pl.semaphore_wait(barrier, len(BLOCKS))
    start(0, lambda b: r0_out, r0_in, -1)
    for j in range(AT + ST):
        inverse[j : j + 1, :] = jnp.sum(found_by[j], axis=0, keepdims=True)

    def geometry(ahead, behind, mass, ahead_new, behind_new):
        bond = [p - q for p, q in zip(ahead, behind)]
        length = jnp.maximum(
            jnp.sqrt(bond[0] * bond[0] + bond[1] * bond[1] + bond[2] * bond[2]), 0.5
        )
        direction = [b / length for b in bond]
        scale = 1.0 / jnp.sqrt(mass)
        shift = [p - q for p, q in zip(ahead_new, behind_new)]
        right = scale * (
            direction[0] * shift[0] + direction[1] * shift[1] + direction[2] * shift[2] - length
        )
        return length, scale, [scale * d for d in direction], right

    near_data = [e[1] for e in ends]
    _, _, tree_gain, tree_right = geometry(
        head_data[0:3],
        near_data[0:3],
        head_mass + near_data[6],
        head_new,
        [near_data[i] + near_data[3 + i] for i in range(3)],
    )
    tree_gain = [jnp.where(is_halo, 0.0, g) for g in tree_gain]
    tree_right = jnp.where(is_halo, 0.0, tree_right)

    parent = lookup(
        [inverse[j : j + 1, :] for j in range(AT)], near // LANES, near % LANES
    ).astype(I32)
    has_parent = jnp.logical_and(parent > 0, jnp.logical_not(is_halo))
    parent = jnp.maximum(parent - 1, 0)
    root = jnp.where(is_halo, slot + 1, 0).astype(F32)

    def climb(label):
        above = lookup([label[t : t + 1, :] for t in range(BT)], parent // LANES, parent % LANES)
        return jnp.where(has_parent, above, root)

    def put_kinds(values, out=kinds):
        for k, value in enumerate(values):
            for t in range(BT):
                out[t, k : k + 1, :] = value[t : t + 1, :]

    def times_ones(values, matrix):
        height = (len(values) + 15) // 16 * 16
        put_kinds(values)
        full = jnp.concatenate([kinds[t, :height, :] for t in range(BT)], axis=1)
        high = full.astype(jnp.bfloat16)
        rest = full - high.astype(F32)
        mid = rest.astype(jnp.bfloat16)
        low = (rest - mid.astype(F32)).astype(jnp.bfloat16)
        parts = jnp.concatenate([high, mid, low], axis=0)
        product = jnp.dot(parts, matrix, preferred_element_type=F32)
        return product[:height] + (product[height : 2 * height] + product[2 * height :])

    def keep_sums(total, count):
        height = (count + 7) // 8 * 8
        for j in range(AT):
            sums[j, :height, :] = total[:height, j * LANES : (j + 1) * LANES]

    def to_atoms(weighted):
        keep_sums(times_ones(weighted, incidence[...]), len(weighted))

    def at_near_of(n):
        return lookup([sums[j, n : n + 1, :] for j in range(AT)], near // LANES, near % LANES)

    def difference(n):
        at_head, at_near = at_ends(lambda j: sums[j, n : n + 1, :])
        return head_mass * at_head - near_mass * at_near

    label_one = climb(root)
    child = jnp.logical_and(label_one > 0.0, jnp.logical_not(is_halo))
    label_two = climb(label_one)
    start_of = [jnp.where(child, g, 0.0) for g in tree_gain]
    product = times_ones(
        [tree_right * g for g in tree_gain]
        + [start_of[i] * tree_gain[m] for i, m in PAIRS],
        incidence[...],
    )
    slots = inverse[AT : AT + ST, :].astype(I32)
    slot_bond = jnp.maximum(slots - 1, 0)
    slot_head = lookup(
        [head[t : t + 1, :].astype(F32) for t in range(BT)],
        slot_bond // LANES,
        slot_bond % LANES,
    ).astype(I32)
    slot_atoms = []
    for s in range(ST):
        at = jnp.broadcast_to(slot_head[s : s + 1, :], (8, LANES))
        used = jnp.broadcast_to(slots[s : s + 1, :], (8, LANES)) > 0
        atoms = jnp.zeros((8, LANES), F32)
        for j in range(AT):
            atoms = jnp.where(at // LANES == j, take(table[j], at % LANES), atoms)
        slot_atoms.append(pltpu.roll(jnp.where(used, atoms, 0.0), SEND * 4, axis=1))
    label = climb(climb(label_two))
    to_cols(7, label)
    for s in range(ST):
        number = (lane128[0:1] + (s * LANES + 1)).astype(F32)
        trees_of[:, s * LANES : (s + 1) * LANES] = jnp.where(cols[7] == number, 1.0, 0.0).astype(
            jnp.bfloat16
        )
    keep_sums(product, 9)
    diffs = [difference(n) for n in range(3)]
    tree_next = tree_right - sum(tree_gain[i] * diffs[i] for i in range(3))
    below = {
        pair: head_mass * (start_of[pair[0]] * tree_gain[pair[1]]) - near_mass * at_near_of(3 + n)
        for n, pair in enumerate(PAIRS)
    }
    start_next = [
        start_of[i] - sum(tree_gain[m] * below[min(i, m), max(i, m)] for m in range(3))
        for i in range(3)
    ]
    tree_sums = times_ones(
        [start_of[i] * start_of[m] for i, m in PAIRS]
        + [start_of[i] * start_next[m] for i, m in PAIRS]
        + [start_next[i] * start_next[m] for i, m in PAIRS]
        + [y * tree_right for y in start_of]
        + [y * tree_next for y in start_of]
        + [y * tree_next for y in start_next],
        trees_of[...],
    )
    for s in range(ST):
        groups = [tree_sums[8 * n : 8 * n + 8, s * LANES : (s + 1) * LANES] for n in range(4)]
        turned = [pltpu.roll(g, SEND * n, axis=1) if n else g for n, g in enumerate(groups)]
        turned.append(slot_atoms[s])
        for b in BLOCKS:
            if b // 8 == s:
                out = turned[0]
                for n in range(1, len(turned)):
                    out = jnp.where(group8 == (b + n) % 8, turned[n], out)
                a_out[ROW_OF[b]] = out
    start(1, lambda b: a_out.at[ROW_OF[b]], a_in, 1)
    to_atoms([tree_next * g for g in tree_gain])
    diffs = [difference(n) for n in range(3)]
    tree_last = tree_next - sum(tree_gain[i] * diffs[i] for i in range(3))
    tree_sums = times_ones([y * tree_last for y in start_next], trees_of[...])
    for s in range(ST):
        a2_out[s] = tree_sums[0:4, s * LANES : (s + 1) * LANES]
    start(2, lambda b: a2_out.at[b // 8], a2_in, 1)

    def merge(source, width, turn=0):
        tiles = []
        for tile in range(ST):
            out = jnp.zeros((width, LANES), F32)
            for b in BLOCKS:
                if b // 8 == tile:
                    out = jnp.where(group8[:width] == (b + turn) % 8, source[ROW_OF[b]], out)
            if turn:
                out = pltpu.roll(out, LANES - SEND * turn, axis=1)
            tiles.append(out)
        return tiles

    to_cols(2, head_mass)
    to_cols(3, near_mass)

    def shared_rows(t, carry):
        for part in range(2):
            here = pl.ds(pl.multiple_of(t * 64 + part * 32, 32), 32)
            heads, tails = cols[0, here, :], cols[1, here, :]
            masses, near_masses = cols[2, here, :], cols[3, here, :]
            minus_near = -near_masses
            for u in range(BT):
                head_row, tail_row = rows[0, u : u + 1, :], rows[1, u : u + 1, :]
                coupling[here, u * LANES : (u + 1) * LANES] = jnp.where(
                    tails == head_row, minus_near, jnp.where(tails == tail_row, near_masses, 0.0)
                ) - jnp.where(heads == tail_row, masses, 0.0)
        return carry

    lax.fori_loop(0, BONDS // 64, shared_rows, 0)
    all_of(0, r0_in).wait_recv()
    halo = merge(r0_in, 8)
    slot_tile, slot_lane = slot // LANES, slot % LANES
    tail_data = []
    for k in range(7):
        far = lookup([halo[s][k : k + 1, :] for s in range(ST)], slot_tile, slot_lane)
        tail_data.append(jnp.where(is_halo, far, near_data[k]))
    tail_new = [tail_data[i] + tail_data[3 + i] for i in range(3)]
    length, scale, gain, right = geometry(
        head_data[0:3], tail_data[0:3], head_mass + tail_data[6], head_new, tail_new
    )
    own = 1.0 - head_mass * (gain[0] * gain[0] + gain[1] * gain[1] + gain[2] * gain[2])
    high = [g.astype(half).astype(F32) for g in gain]
    mid = [(g - h).astype(half).astype(F32) for g, h in zip(gain, high)]
    low = [(g - h - m).astype(half).astype(F32) for g, h, m in zip(gain, high, mid)]
    put_kinds(high + mid + low + high + mid + high, split.at[0])
    right_side = jnp.concatenate([split[0, t] for t in range(BT)], axis=1).astype(half)
    put_kinds(high + high + high + mid + mid + low, split.at[1])
    for t in range(BT):
        left_side[t * LANES : (t + 1) * LANES, :] = jnp.transpose(split[1, t]).astype(half)

    for t in range(BT):
        here = slice(t * LANES, (t + 1) * LANES)
        dots = jnp.dot(left_side[here, :], right_side, preferred_element_type=F32)
        coupling[here, :] = coupling[here, :] * dots

    def couple(values):
        for n, value in enumerate(values):
            vec[n] = value
        outs = [[] for _ in values]
        for t in range(BT):
            for n in range(len(values)):
                total = None
                for u in range(BT):
                    part = (
                        coupling[t * LANES : (t + 1) * LANES, u * LANES : (u + 1) * LANES]
                        * vec[n, u : u + 1, :]
                    )
                    total = part if total is None else total + part
                col = jnp.sum(total, axis=1, keepdims=True)
                outs[n].append(jnp.sum(jnp.where(eye, col, 0.0), axis=0, keepdims=True))
        return [own * v - jnp.concatenate(o, axis=0) for v, o in zip(values, outs)]

    def by_kind(tiles, count):
        for s in range(ST):
            kinds[s, 0 : tiles[s].shape[0], :] = tiles[s]
        return [
            jnp.concatenate([kinds[s, k : k + 1, :] for s in range(ST)], axis=0)
            for k in range(count)
        ]

    def over_senders(values):
        lines = [jnp.sum(v, axis=0, keepdims=True) for v in values]
        lines += [jnp.zeros((1, LANES), F32)] * (-len(lines) % 8)
        block = jnp.concatenate(lines, axis=0)
        turned = [pltpu.roll(block, SEND * n, axis=1) for n in range(1, LANES // SEND)]
        return ((block + turned[0]) + (turned[1] + turned[2])) + (
            (turned[3] + turned[4]) + (turned[5] + turned[6])
        )

    own_mass = mine[6:7, :]

    def solve(sums_of, squares, found, count):
        for k in range(len(found), count):
            now = []
            for i in range(3):
                total = sums_of(k, i)
                for j in range(k):
                    for m in range(3):
                        total = total + squares(k - 1 - j, i, m) * found[j][m]
                now.append(-own_mass * total)
            found.append(now)
        return found

    all_of(1, a_in).wait_recv()
    far = []
    for n in range(5):
        far += by_kind(merge(a_in, 8, n), 8)
    far_head, far_mass = far[32:38], far[38]
    far_new = [far_head[i] + far_head[3 + i] for i in range(3)]
    used = far_mass > 0.0
    far_length, far_scale, far_gain, far_right = geometry(
        far_head[0:3],
        [mine[i : i + 1, :] for i in range(3)],
        far_mass + own_mass,
        far_new,
        [mine[i : i + 1, :] + mine[3 + i : 4 + i, :] for i in range(3)],
    )
    far_gain = [jnp.where(used, g, 0.0) for g in far_gain]
    far_right = jnp.where(used, far_right, 0.0)
    pull = [far_mass * g for g in far_gain]
    far_own = 1.0 - (pull[0] * far_gain[0] + pull[1] * far_gain[1] + pull[2] * far_gain[2])
    turn = []
    for power in range(3):
        form = far[6 * power : 6 * power + 6]
        turn.append(
            sum(
                pull[i] * sum(pull[m] * form[PAIRS.index((min(i, m), max(i, m)))] for m in range(3))
                for i in range(3)
            )
        )
    feed = [sum(pull[i] * far[18 + 3 * k + i] for i in range(3)) for k in range(3)]
    far_chain = [far_right]

    def next_chain():
        k = len(far_chain) - 1
        value = far_own * far_chain[k] + feed[k]
        for j in range(k):
            value = value + turn[k - 1 - j] * far_chain[j]
        far_chain.append(value)

    for _ in range(3):
        next_chain()
    far_reach = [far_own]
    far_reach.append(far_own * far_own + turn[0])
    far_reach.append(far_own * far_reach[1] + turn[0] * far_own + turn[1])
    lists = [far_gain[i] * far_chain[k] for k in range(4) for i in range(3)]
    squares_of = [far_gain[i] * far_gain[m] for i, m in PAIRS]
    lists += squares_of + [q * far_reach[n] for n in range(3) for q in squares_of]
    block = over_senders(lists)

    def squares(power, i, m):
        at = 12 + power * 6 + PAIRS.index((min(i, m), max(i, m)))
        return block[at : at + 1, :]

    found = solve(lambda k, i: block[3 * k + i : 3 * k + i + 1, :], squares, [], 4)
    for k in range(4):
        z = sum(far_gain[i] * found[k][i] for i in range(3))
        for s in range(ST):
            b_out[s, k : k + 1, :] = z[s : s + 1, :]
    start(3, lambda b: b_out.at[b // 8], b_in, -1)


    atom_bond = inverse[0:16, :].astype(I32)
    bond_at = jnp.maximum(atom_bond - 1, 0)
    atom_label = lookup([label[t : t + 1, :] for t in range(BT)], bond_at // LANES, bond_at % LANES)
    row16 = lax.broadcasted_iota(I32, (16, LANES), 0)
    atom_label = jnp.where(
        jnp.logical_and(atom_bond > 0, row16 < AT), atom_label, 0.0
    ).astype(I32)
    label = label.astype(I32)

    def labelled(tiles, which):
        at = jnp.maximum(which - 1, 0)
        return jnp.where(which > 0, lookup(tiles, at // LANES, at % LANES), 0.0)

    unit = jnp.where(is_halo, 1.0, 0.0)
    chain, reach = [right], [unit]
    for _ in range(4):
        nxt = couple([chain[-1], reach[-1]])
        chain.append(nxt[0])
        reach.append(nxt[1])
    base = chain[0] + chain[1] + chain[2] + chain[3] + chain[4]
    grown = [reach[0]]
    for m in range(1, 5):
        grown.append(grown[-1] + reach[m])
    to_atoms([v * g for v in [base] + grown[:4] for g in gain])
    moves = []
    for n in range(15):
        moves.append(difference(n))
    all_of(3, b_in).wait_recv()
    back = merge(b_in, 4)

    def kind_rows(tiles, k):
        return [tiles[s][k : k + 1, :] for s in range(ST)]

    z = [labelled(kind_rows(back, k), label) for k in range(4)]
    sol_one = base
    for j in range(4):
        sol_one = sol_one + z[j] * grown[3 - j]
    current = None
    moved = []
    for i in range(3):
        ahead = head_new[i] - jnp.where(is_halo, 0.0, tail_new[i])
        step = moves[i]
        for j in range(4):
            step = step + z[j] * moves[3 * (1 + 3 - j) + i]
        stretch = ahead - step
        moved.append(stretch)
        current = stretch * stretch if current is None else current + stretch * stretch

    def second_right(scale, length, current):
        target = jnp.sqrt(jnp.maximum(2.0 * length * length - current, 0.5 * length * length))
        return scale * (length - target)

    chain_two = [jnp.where(is_halo, 0.0, second_right(scale, length, current))]
    tree_sums = times_ones(
        [reach[k] * chain_two[0] for k in range(1, 5)] + [unit * m for m in moved],
        trees_of[...],
    )
    for s in range(ST):
        c_out[s] = tree_sums[0:8, s * LANES : (s + 1) * LANES]
    start(4, lambda b: c_out.at[b // 8], c_in, 1)
    for _ in range(4):
        chain_two.append(couple([chain_two[-1]])[0])

    for n in range(15):
        for j in range(AT):
            gathered[n, j : j + 1, :] = sums[j, n : n + 1, :]
        gathered[n, AT:16, :] = jnp.zeros((16 - AT, LANES), F32)
    base_two = chain_two[0] + chain_two[1] + chain_two[2] + chain_two[3] + chain_two[4]
    to_atoms([v * g for v in (base_two, grown[4]) for g in gain])
    mass_atoms = jnp.concatenate(
        [table[j, 6:7, :] for j in range(AT)] + [jnp.zeros((16 - AT, LANES), F32)], axis=0
    )
    still = []
    for i in range(3):
        spread_base = jnp.concatenate(
            [gathered[i, j : j + 1, :] + sums[j, i : i + 1, :] for j in range(AT)]
            + [jnp.zeros((16 - AT, LANES), F32)],
            axis=0,
        )
        start_pos = jnp.concatenate(
            [table[j, i : i + 1, :] + table[j, 3 + i : 4 + i, :] for j in range(AT)]
            + [jnp.zeros((16 - AT, LANES), F32)],
            axis=0,
        )
        still.append(start_pos - mass_atoms * spread_base)
    trees = [[mass_atoms * gathered[3 * (1 + n) + i] for i in range(3)] for n in range(4)]
    no_atoms = jnp.zeros((16 - AT, LANES), F32)
    trees.append(
        [
            mass_atoms
            * jnp.concatenate([sums[j, 3 + i : 4 + i, :] for j in range(AT)] + [no_atoms], axis=0)
            for i in range(3)
        ]
    )
    all_of(2, a2_in).wait_recv()
    late = by_kind(merge(a2_in, 4), 3)
    feed.append(sum(pull[i] * late[i] for i in range(3)))
    next_chain()
    far_reach.append(
        far_own * far_reach[2] + turn[0] * far_reach[1] + turn[1] * far_own + turn[2]
    )
    last_sum = over_senders([far_gain[i] * far_chain[4] for i in range(3)])
    solve(lambda k, i: last_sum[i : i + 1, :], squares, found, 5)
    sent_total = [
        found[0][i] + found[1][i] + found[2][i] + found[3][i] + found[4][i] for i in range(3)
    ]
    sent_moved = [mine[i : i + 1, :] + mine[3 + i : 4 + i, :] - sent_total[i] for i in range(3)]
    number16 = row16 * LANES + lax.broadcasted_iota(I32, (16, LANES), 1)
    which = jnp.zeros((16, LANES), I32)
    for e in range(SEND):
        which = jnp.where(number16 == sent8[0:1, e : e + 1], e + 1, which)

    all_of(4, c_in).wait_recv()
    far_two = by_kind(merge(c_in, 8), 7)
    apart = [far_two[4 + i] - sent_moved[i] for i in range(3)]
    far_right_two = second_right(
        far_scale, far_length, apart[0] * apart[0] + apart[1] * apart[1] + apart[2] * apart[2]
    )
    far_right_two = jnp.where(used, far_right_two, 0.0)
    far_chain_two = [far_right_two]
    for k in range(4):
        far_chain_two.append(far_two[k] + far_reach[k] * far_right_two)
    block_two = over_senders([far_gain[i] * far_chain_two[k] for k in range(5) for i in range(3)])
    found_two = solve(lambda k, i: block_two[3 * k + i : 3 * k + i + 1, :], squares, [], 5)
    for k in range(4):
        z_two = sum(far_gain[i] * found_two[k][i] for i in range(3))
        for s in range(ST):
            d_out[s, k : k + 1, :] = z_two[s : s + 1, :]
    for s in range(ST):
        d_out[s, 4:5, :] = far_right_two[s : s + 1, :]
        d_out[s, 5:8, :] = jnp.zeros((3, LANES), F32)
    start(5, lambda b: d_out.at[b // 8], d_in, -1)

    for i in range(3):
        total = sent_total[i]
        for k in range(5):
            total = total + found_two[k][i]
        own_move = take(jnp.broadcast_to(total, (16, LANES)), jnp.maximum(which - 1, 0))
        still[i] = still[i] - jnp.where(which > 0, own_move, 0.0)

    all_of(5, d_in).wait_recv()
    last = merge(d_in, 8)
    result = sol_one + base_two
    for j in range(5):
        result = result + labelled(kind_rows(last, j), label) * grown[3 - j if j < 4 else 4]
    for t in range(BT):
        mult_ref[:, t * LANES : (t + 1) * LANES] = result[t : t + 1, :]
    both = [[back[s][k : k + 1, :] + last[s][k : k + 1, :] for s in range(ST)] for k in range(4)]
    both.append(kind_rows(last, 4))
    for j in range(5):
        z_atom = labelled(both[j], atom_label)
        for i in range(3):
            still[i] = still[i] - z_atom * trees[3 - j if j < 4 else 4][i]
    for i in range(3):
        for j in range(AT):
            at = i * ATOMS + j * LANES
            new_ref[:, at : at + LANES] = still[i][j : j + 1, :]

    for stage, target in ((0, r0_in), (1, a_in), (2, a2_in), (3, b_in), (4, c_in), (5, d_in)):
        all_of(stage, target).wait_send()


def write_out(new_ref, mult_ref, new_out, mult_out):
    new_out[...] = new_ref[...]
    mult_out[...] = mult_ref[...]


def solution(mesh):
    sizes = tuple(mesh.shape[n] for n in ("gx", "gy", "gz"))

    def per_device(old_pos, displacement, inv_mass, bond_head, bond_tail, send_list):
        near = len(BLOCKS)
        vmem = pl.BlockSpec(memory_space=pltpu.VMEM)
        new_pos, multipliers = pl.pallas_call(
            functools.partial(kernel, sizes),
            out_shape=(pltpu.VMEM((1, 3 * ATOMS), F32), pltpu.VMEM((1, BONDS), F32)),
            in_specs=[pl.BlockSpec(memory_space=pl.ANY)] * 6,
            out_specs=(vmem, vmem),
            scratch_shapes=[
                pltpu.VMEM((3, 1, ATOMS), F32),
                pltpu.VMEM((3, 1, ATOMS), F32),
                pltpu.VMEM((1, ATOMS), F32),
                pltpu.VMEM((1, BONDS), I32),
                pltpu.VMEM((1, BONDS), I32),
                pltpu.VMEM((1, SEND), I32),
                pltpu.SemaphoreType.DMA((6,)),
                pltpu.VMEM((AT, 8, LANES), F32),
                pltpu.VMEM((2, 8, LANES), I32),
                pltpu.VMEM((8, BONDS, LANES), F32),
                pltpu.VMEM((BONDS, ATOMS), jnp.bfloat16),
                pltpu.VMEM((BONDS, ST * LANES), jnp.bfloat16),
                pltpu.VMEM((BONDS, BONDS), F32),
                pltpu.VMEM((AT + ST, 8, LANES), F32),
                pltpu.VMEM((AT + ST, LANES), F32),
                pltpu.VMEM((2, 8, LANES), F32),
                pltpu.VMEM((2, 8, LANES), F32),
                pltpu.VMEM((2, BT, 32, LANES), F32),
                pltpu.VMEM((BONDS, 32), jnp.bfloat16),
                pltpu.VMEM((AT, 16, LANES), F32),
                pltpu.VMEM((8, 40, LANES), F32),
                pltpu.VMEM((15, 16, LANES), F32),
                pltpu.VMEM((8, LANES), F32),
                pltpu.VMEM((near, 8, LANES), F32),
                pltpu.VMEM((ST, 4, LANES), F32),
                pltpu.VMEM((ST, 4, LANES), F32),
                pltpu.VMEM((ST, 8, LANES), F32),
                pltpu.VMEM((ST, 8, LANES), F32),
                pltpu.VMEM((near, 8, LANES), F32),
                pltpu.VMEM((near, 8, LANES), F32),
                pltpu.VMEM((near, 4, LANES), F32),
                pltpu.VMEM((near, 4, LANES), F32),
                pltpu.VMEM((near, 8, LANES), F32),
                pltpu.VMEM((near, 8, LANES), F32),
                pltpu.SemaphoreType.DMA((6,)),
                pltpu.SemaphoreType.DMA((6,)),
            ],
            compiler_params=pltpu.CompilerParams(collective_id=0, has_side_effects=True),
        )(
            old_pos.reshape(3, 1, ATOMS),
            displacement.reshape(3, 1, ATOMS),
            inv_mass.reshape(1, ATOMS),
            bond_head.reshape(1, BONDS),
            bond_tail.reshape(1, BONDS),
            send_list.reshape(1, SEND),
        )
        new_pos, multipliers = pl.pallas_call(
            write_out,
            out_shape=(
                jax.ShapeDtypeStruct((1, 3 * ATOMS), F32),
                jax.ShapeDtypeStruct((1, BONDS), F32),
            ),
            in_specs=[vmem] * 2,
            out_specs=(vmem, vmem),
        )(
            pltpu.with_memory_space_constraint(new_pos, pltpu.VMEM),
            pltpu.with_memory_space_constraint(multipliers, pltpu.VMEM),
        )
        return new_pos.reshape(old_pos.shape), multipliers.reshape(bond_head.shape)

    return jax.shard_map(
        per_device,
        mesh=mesh,
        in_specs=(
            P(None, "gx", "gy", "gz", None),
            P(None, "gx", "gy", "gz", None),
            P("gx", "gy", "gz", None),
            P("gx", "gy", "gz", None),
            P("gx", "gy", "gz", None),
            P("gx", "gy", "gz", None),
        ),
        out_specs=(P(None, "gx", "gy", "gz", None), P("gx", "gy", "gz", None)),
        check_vma=False,
    )
```

```python
import functools

import jax
import jax.numpy as jnp
from jax import lax
from jax.experimental import pallas as pl
from jax.experimental.pallas import tpu as pltpu
from jax.sharding import PartitionSpec as P

MESH = pl.DeviceIdType.MESH
ATOMS = 1536
BONDS = 1024
SEND = 16
LANES = 128
AT = ATOMS // LANES
BT = BONDS // LANES
ST = 4
BLOCKS = [b for b in range(27) if b != 13]
ROW_OF = {b: n for n, b in enumerate(BLOCKS)}
FAR_FIRST = sorted(BLOCKS, key=lambda b: (b // 9 == 1) + (b // 3 % 3 == 1) + (b % 3 == 1))
F32 = jnp.float32
I32 = jnp.int32
PAIRS = [(0, 0), (0, 1), (0, 2), (1, 1), (1, 2), (2, 2)]


def take(rows, lane):
    numbers = lax.GatherDimensionNumbers(
        offset_dims=(),
        collapsed_slice_dims=(1,),
        start_index_map=(1,),
        operand_batching_dims=(0,),
        start_indices_batching_dims=(0,),
    )
    return lax.gather(
        rows, lane[..., None], numbers, (1, 1), mode=lax.GatherScatterMode.PROMISE_IN_BOUNDS
    )


def lookup(tiles, tile, lane):
    out = jnp.zeros(lane.shape, F32)
    for j, row in enumerate(tiles):
        out = jnp.where(tile == j, take(jnp.broadcast_to(row, lane.shape), lane), out)
    return out


def kernel(
    sizes,
    old_hbm,
    move_hbm,
    mass_hbm,
    head_hbm,
    tail_hbm,
    send_hbm,
    new_ref,
    mult_ref,
    old_ref,
    move_ref,
    mass_ref,
    head_ref,
    tail_ref,
    send_ref,
    load_sem,
    table,
    idx,
    cols,
    incidence,
    trees_of,
    coupling,
    found_by,
    inverse,
    vec,
    rows,
    split,
    left_side,
    sums,
    kinds,
    gathered,
    r0_out,
    a_out,
    a2_out,
    b_out,
    c_out,
    d_out,
    r0_in,
    a_in,
    a2_in,
    b_in,
    c_in,
    d_in,
    send_sem,
    recv_sem,
):
    loads = [
        pltpu.make_async_copy(source, target, load_sem.at[n])
        for n, (source, target) in enumerate(
            (
                (send_hbm, send_ref),
                (old_hbm, old_ref),
                (move_hbm, move_ref),
                (mass_hbm, mass_ref),
                (head_hbm, head_ref),
                (tail_hbm, tail_ref),
            )
        )
    ]
    for load in loads:
        load.start()
    names = ("gx", "gy", "gz")
    me = [lax.axis_index(n) for n in names]

    near_by = [{o: lax.rem(m + o + n, n) if o else m for o in (-1, 0, 1)} for m, n in zip(me, sizes)]

    def device(block, sign):
        offs = (block // 9 - 1, block // 3 % 3 - 1, block % 3 - 1)
        return tuple(axis[sign * o] for axis, o in zip(near_by, offs))

    barrier = pltpu.get_barrier_semaphore()
    for b in BLOCKS:
        pl.semaphore_signal(barrier, inc=1, device_id=device(b, 1), device_id_type=MESH)

    def start(stage, source, target, sign):
        for b in FAR_FIRST:
            pltpu.make_async_remote_copy(
                src_ref=source(b),
                dst_ref=target.at[ROW_OF[b]],
                send_sem=send_sem.at[stage],
                recv_sem=recv_sem.at[stage],
                device_id=device(b, sign),
                device_id_type=MESH,
            ).start()

    def all_of(stage, target):
        return pltpu.make_async_remote_copy(
            src_ref=target,
            dst_ref=target,
            send_sem=send_sem.at[stage],
            recv_sem=recv_sem.at[stage],
            device_id=device(0, 1),
            device_id_type=MESH,
        )

    lane8 = lax.broadcasted_iota(I32, (8, LANES), 1)
    group8 = lane8 // SEND
    sub128 = lax.broadcasted_iota(I32, (LANES, LANES), 0)
    lane128 = lax.broadcasted_iota(I32, (LANES, LANES), 1)
    eye = sub128 == lane128

    for load in loads:
        load.wait()
    for j in range(AT):
        cut = pl.ds(j * LANES, LANES)
        for i in range(3):
            table[j, i : i + 1, :] = old_ref[i, :, cut]
            table[j, 3 + i : 4 + i, :] = move_ref[i, :, cut]
        table[j, 6:7, :] = mass_ref[:, cut]
        table[j, 7:8, :] = jnp.zeros((1, LANES), F32)
    sent8 = jnp.broadcast_to(
        jnp.concatenate([send_ref[...]] * (LANES // SEND), axis=1), (8, LANES)
    )
    mine = jnp.zeros((8, LANES), F32)
    for j in range(AT):
        mine = jnp.where(sent8 // LANES == j, take(table[j], sent8 % LANES), mine)
    r0_out[...] = mine

    for t in range(BT):
        cut = pl.ds(t * LANES, LANES)
        idx[0, t : t + 1, :] = head_ref[:, cut]
        idx[1, t : t + 1, :] = tail_ref[:, cut]
    head = idx[0]
    tail = idx[1]
    is_halo = tail >= ATOMS
    slot = jnp.where(is_halo, tail - ATOMS, 0)
    near = jnp.where(is_halo, 0, tail)

    def at_ends(row):
        lines = [row(j) for j in range(AT)]
        return (
            lookup(lines, head // LANES, head % LANES),
            lookup(lines, near // LANES, near % LANES),
        )

    ends = [at_ends(lambda j, k=k: table[j, k : k + 1, :]) for k in range(7)]
    head_mass = ends[6][0]
    near_mass = jnp.where(is_halo, 0.0, ends[6][1])
    head_data = [e[0] for e in ends]
    head_new = [head_data[i] + head_data[3 + i] for i in range(3)]

    def to_cols(k, value):
        for t in range(BT):
            col = jnp.sum(jnp.where(eye, value[t : t + 1, :], 0.0), axis=1, keepdims=True)
            cols[k, t * LANES : (t + 1) * LANES, :] = jnp.broadcast_to(col, (LANES, LANES))

    rows[0] = head.astype(F32)
    rows[1] = tail.astype(F32)
    both_ends = rows[0] * 2048.0 + rows[1]
    for t in range(BT):
        here = slice(t * LANES, (t + 1) * LANES)
        col = jnp.sum(jnp.where(eye, both_ends[t : t + 1, :], 0.0), axis=1, keepdims=True)
        col = jnp.broadcast_to(col, (LANES, LANES))
        heads = jnp.floor(col * (1.0 / 2048.0))
        for k, value in enumerate((heads, col - 2048.0 * heads)):
            cols[k, here, :] = value

    found_by[...] = jnp.zeros(found_by.shape, F32)
    kinds[...] = jnp.zeros(kinds.shape, F32)
    split[...] = jnp.zeros(split.shape, F32)
    half = jnp.bfloat16

    def incidence_rows(t, carry):
        here = pl.ds(pl.multiple_of(t * LANES, LANES), LANES)
        heads = cols[0, here, :]
        tails = cols[1, here, :]
        number = (sub128 + (t * LANES + 1)).astype(F32)
        atoms = [(lane8 + j * LANES).astype(F32) for j in range(AT + ST)]
        numbers_of = [found_by[j] for j in range(AT + ST)]
        for pair in range(LANES // 16):
            cuts = [slice(16 * pair + 8 * r, 16 * pair + 8 * r + 8) for r in range(2)]
            for j in range(AT + ST):
                parts = []
                for cut in cuts:
                    if j < AT:
                        found = heads[cut] == atoms[j]
                        parts.append(
                            jnp.where(found, 1.0, jnp.where(tails[cut] == atoms[j], -1.0, 0.0))
                        )
                    else:
                        found = tails[cut] == atoms[j]
                    numbers_of[j] = jnp.where(found, number[cut], numbers_of[j])
                if j < AT:
                    at = pl.ds(pl.multiple_of(t * LANES + pair * 16, 16), 16)
                    incidence[at, j * LANES : (j + 1) * LANES] = jnp.concatenate(
                        parts, axis=0
                    ).astype(half)
        for j in range(AT + ST):
            found_by[j] = numbers_of[j]
        return carry

    lax.fori_loop(0, BT, incidence_rows, 0)
    for j in range(AT + ST):
        inverse[j : j + 1, :] = jnp.sum(found_by[j], axis=0, keepdims=True)

    def geometry(ahead, behind, mass, ahead_new, behind_new):
        bond = [p - q for p, q in zip(ahead, behind)]
        length = jnp.maximum(
            jnp.sqrt(bond[0] * bond[0] + bond[1] * bond[1] + bond[2] * bond[2]), 0.5
        )
        direction = [b / length for b in bond]
        scale = 1.0 / jnp.sqrt(mass)
        shift = [p - q for p, q in zip(ahead_new, behind_new)]
        right = scale * (
            direction[0] * shift[0] + direction[1] * shift[1] + direction[2] * shift[2] - length
        )
        return length, scale, [scale * d for d in direction], right

    near_data = [e[1] for e in ends]
    _, _, tree_gain, tree_right = geometry(
        head_data[0:3],
        near_data[0:3],
        head_mass + near_data[6],
        head_new,
        [near_data[i] + near_data[3 + i] for i in range(3)],
    )
    tree_gain = [jnp.where(is_halo, 0.0, g) for g in tree_gain]
    tree_right = jnp.where(is_halo, 0.0, tree_right)

    parent = lookup(
        [inverse[j : j + 1, :] for j in range(AT)], near // LANES, near % LANES
    ).astype(I32)
    has_parent = jnp.logical_and(parent > 0, jnp.logical_not(is_halo))
    parent = jnp.maximum(parent - 1, 0)
    root = jnp.where(is_halo, slot + 1, 0).astype(F32)

    def climb(label):
        above = lookup([label[t : t + 1, :] for t in range(BT)], parent // LANES, parent % LANES)
        return jnp.where(has_parent, above, root)

    def put_kinds(values, out=kinds):
        for k, value in enumerate(values):
            out[:, k, :] = value

    def times_ones(values, matrix):
        height = (len(values) + 15) // 16 * 16
        put_kinds(values)
        full = jnp.concatenate([kinds[t, :height, :] for t in range(BT)], axis=1)
        high = full.astype(jnp.bfloat16)
        rest = full - high.astype(F32)
        mid = rest.astype(jnp.bfloat16)
        low = (rest - mid.astype(F32)).astype(jnp.bfloat16)
        parts = jnp.concatenate([high, mid, low], axis=0)
        product = jnp.dot(parts, matrix, preferred_element_type=F32)
        return product[:height] + (product[height : 2 * height] + product[2 * height :])

    def keep_sums(total, count):
        height = (count + 7) // 8 * 8
        for j in range(AT):
            sums[j, :height, :] = total[:height, j * LANES : (j + 1) * LANES]

    def to_atoms(weighted):
        keep_sums(times_ones(weighted, incidence[...]), len(weighted))

    def at_near_of(n):
        return lookup([sums[j, n : n + 1, :] for j in range(AT)], near // LANES, near % LANES)

    def difference(n):
        at_head, at_near = at_ends(lambda j: sums[j, n : n + 1, :])
        return head_mass * at_head - near_mass * at_near

    label_one = climb(root)
    child = jnp.logical_and(label_one > 0.0, jnp.logical_not(is_halo))
    label_two = climb(label_one)
    start_of = [jnp.where(child, g, 0.0) for g in tree_gain]
    product = times_ones(
        [tree_right * g for g in tree_gain]
        + [start_of[i] * tree_gain[m] for i, m in PAIRS],
        incidence[...],
    )
    pl.semaphore_wait(barrier, len(BLOCKS))
    start(0, lambda b: r0_out, r0_in, -1)
    slots = inverse[AT : AT + ST, :].astype(I32)
    slot_bond = jnp.maximum(slots - 1, 0)
    slot_head = lookup(
        [head[t : t + 1, :].astype(F32) for t in range(BT)],
        slot_bond // LANES,
        slot_bond % LANES,
    ).astype(I32)
    slot_atoms = []
    for s in range(ST):
        at = jnp.broadcast_to(slot_head[s : s + 1, :], (8, LANES))
        used = jnp.broadcast_to(slots[s : s + 1, :], (8, LANES)) > 0
        atoms = jnp.zeros((8, LANES), F32)
        for j in range(AT):
            atoms = jnp.where(at // LANES == j, take(table[j], at % LANES), atoms)
        slot_atoms.append(pltpu.roll(jnp.where(used, atoms, 0.0), SEND * 4, axis=1))
    label = climb(climb(label_two))
    to_cols(7, label)
    for s in range(ST):
        number = (lane128[0:1] + (s * LANES + 1)).astype(F32)
        trees_of[:, s * LANES : (s + 1) * LANES] = jnp.where(cols[7] == number, 1.0, 0.0).astype(
            jnp.bfloat16
        )
    keep_sums(product, 9)
    diffs = [difference(n) for n in range(3)]
    tree_next = tree_right - sum(tree_gain[i] * diffs[i] for i in range(3))
    below = {
        pair: head_mass * (start_of[pair[0]] * tree_gain[pair[1]]) - near_mass * at_near_of(3 + n)
        for n, pair in enumerate(PAIRS)
    }
    start_next = [
        start_of[i] - sum(tree_gain[m] * below[min(i, m), max(i, m)] for m in range(3))
        for i in range(3)
    ]
    tree_sums = times_ones(
        [start_of[i] * start_of[m] for i, m in PAIRS]
        + [start_of[i] * start_next[m] for i, m in PAIRS]
        + [start_next[i] * start_next[m] for i, m in PAIRS]
        + [y * tree_right for y in start_of]
        + [y * tree_next for y in start_of]
        + [y * tree_next for y in start_next],
        trees_of[...],
    )
    for s in range(ST):
        groups = [tree_sums[8 * n : 8 * n + 8, s * LANES : (s + 1) * LANES] for n in range(4)]
        turned = [pltpu.roll(g, SEND * n, axis=1) if n else g for n, g in enumerate(groups)]
        turned.append(slot_atoms[s])
        for b in BLOCKS:
            if b // 8 == s:
                out = turned[0]
                for n in range(1, len(turned)):
                    out = jnp.where(group8 == (b + n) % 8, turned[n], out)
                a_out[ROW_OF[b]] = out
    start(1, lambda b: a_out.at[ROW_OF[b]], a_in, 1)
    to_atoms([tree_next * g for g in tree_gain])
    diffs = [difference(n) for n in range(3)]
    tree_last = tree_next - sum(tree_gain[i] * diffs[i] for i in range(3))
    tree_sums = times_ones([y * tree_last for y in start_next], trees_of[...])
    for s in range(ST):
        a2_out[s] = tree_sums[0:4, s * LANES : (s + 1) * LANES]
    start(2, lambda b: a2_out.at[b // 8], a2_in, 1)

    def merge(source, width, turn=0):
        tiles = []
        for tile in range(ST):
            out = jnp.zeros((width, LANES), F32)
            for b in BLOCKS:
                if b // 8 == tile:
                    out = jnp.where(group8[:width] == (b + turn) % 8, source[ROW_OF[b]], out)
            if turn:
                out = pltpu.roll(out, LANES - SEND * turn, axis=1)
            tiles.append(out)
        return tiles

    to_cols(2, head_mass)
    to_cols(3, near_mass)

    def shared_rows(t, carry):
        for part in range(2):
            here = pl.ds(pl.multiple_of(t * 64 + part * 32, 32), 32)
            heads, tails = cols[0, here, :], cols[1, here, :]
            masses, near_masses = cols[2, here, :], cols[3, here, :]
            minus_near = -near_masses
            for u in range(BT):
                head_row, tail_row = rows[0, u : u + 1, :], rows[1, u : u + 1, :]
                coupling[here, u * LANES : (u + 1) * LANES] = jnp.where(
                    tails == head_row, minus_near, jnp.where(tails == tail_row, near_masses, 0.0)
                ) - jnp.where(heads == tail_row, masses, 0.0)
        return carry

    lax.fori_loop(0, BONDS // 64, shared_rows, 0)
    all_of(0, r0_in).wait_recv()
    halo = merge(r0_in, 8)
    slot_tile, slot_lane = slot // LANES, slot % LANES
    tail_data = []
    for k in range(7):
        far = lookup([halo[s][k : k + 1, :] for s in range(ST)], slot_tile, slot_lane)
        tail_data.append(jnp.where(is_halo, far, near_data[k]))
    tail_new = [tail_data[i] + tail_data[3 + i] for i in range(3)]
    length, scale, gain, right = geometry(
        head_data[0:3], tail_data[0:3], head_mass + tail_data[6], head_new, tail_new
    )
    own = 1.0 - head_mass * (gain[0] * gain[0] + gain[1] * gain[1] + gain[2] * gain[2])
    high = [g.astype(half).astype(F32) for g in gain]
    mid = [(g - h).astype(half).astype(F32) for g, h in zip(gain, high)]
    low = [(g - h - m).astype(half).astype(F32) for g, h, m in zip(gain, high, mid)]
    put_kinds(high + mid + low + high + mid + high, split.at[0])
    right_side = jnp.concatenate([split[0, t] for t in range(BT)], axis=1).astype(half)
    put_kinds(high + high + high + mid + mid + low, split.at[1])
    for t in range(BT):
        left_side[t * LANES : (t + 1) * LANES, :] = jnp.transpose(split[1, t]).astype(half)

    for t in range(BT):
        here = slice(t * LANES, (t + 1) * LANES)
        dots = jnp.dot(left_side[here, :], right_side, preferred_element_type=F32)
        coupling[here, :] = coupling[here, :] * dots

    def couple(values):
        for n, value in enumerate(values):
            vec[n] = value
        outs = [[] for _ in values]
        for t in range(BT):
            for n in range(len(values)):
                total = None
                for u in range(BT):
                    part = (
                        coupling[t * LANES : (t + 1) * LANES, u * LANES : (u + 1) * LANES]
                        * vec[n, u : u + 1, :]
                    )
                    total = part if total is None else total + part
                col = jnp.sum(total, axis=1, keepdims=True)
                outs[n].append(jnp.sum(jnp.where(eye, col, 0.0), axis=0, keepdims=True))
        return [own * v - jnp.concatenate(o, axis=0) for v, o in zip(values, outs)]

    def by_kind(tiles, count):
        for s in range(ST):
            kinds[s, 0 : tiles[s].shape[0], :] = tiles[s]
        return [kinds[0:ST, k, :] for k in range(count)]

    def over_senders(values):
        lines = [jnp.sum(v, axis=0, keepdims=True) for v in values]
        lines += [jnp.zeros((1, LANES), F32)] * (-len(lines) % 8)
        block = jnp.concatenate(lines, axis=0)
        turned = [pltpu.roll(block, SEND * n, axis=1) for n in range(1, LANES // SEND)]
        return ((block + turned[0]) + (turned[1] + turned[2])) + (
            (turned[3] + turned[4]) + (turned[5] + turned[6])
        )

    own_mass = mine[6:7, :]

    def solve(sums_of, squares, found, count):
        for k in range(len(found), count):
            now = []
            for i in range(3):
                total = sums_of(k, i)
                for j in range(k):
                    for m in range(3):
                        total = total + squares(k - 1 - j, i, m) * found[j][m]
                now.append(-own_mass * total)
            found.append(now)
        return found

    all_of(1, a_in).wait_recv()
    far = []
    for n in range(5):
        far += by_kind(merge(a_in, 8, n), 8)
    far_head, far_mass = far[32:38], far[38]
    far_new = [far_head[i] + far_head[3 + i] for i in range(3)]
    used = far_mass > 0.0
    far_length, far_scale, far_gain, far_right = geometry(
        far_head[0:3],
        [mine[i : i + 1, :] for i in range(3)],
        far_mass + own_mass,
        far_new,
        [mine[i : i + 1, :] + mine[3 + i : 4 + i, :] for i in range(3)],
    )
    far_gain = [jnp.where(used, g, 0.0) for g in far_gain]
    far_right = jnp.where(used, far_right, 0.0)
    pull = [far_mass * g for g in far_gain]
    far_own = 1.0 - (pull[0] * far_gain[0] + pull[1] * far_gain[1] + pull[2] * far_gain[2])
    turn = []
    for power in range(3):
        form = far[6 * power : 6 * power + 6]
        turn.append(
            sum(
                pull[i] * sum(pull[m] * form[PAIRS.index((min(i, m), max(i, m)))] for m in range(3))
                for i in range(3)
            )
        )
    feed = [sum(pull[i] * far[18 + 3 * k + i] for i in range(3)) for k in range(3)]
    far_chain = [far_right]

    def next_chain():
        k = len(far_chain) - 1
        value = far_own * far_chain[k] + feed[k]
        for j in range(k):
            value = value + turn[k - 1 - j] * far_chain[j]
        far_chain.append(value)

    for _ in range(3):
        next_chain()
    far_reach = [far_own]
    far_reach.append(far_own * far_own + turn[0])
    far_reach.append(far_own * far_reach[1] + turn[0] * far_own + turn[1])
    lists = [far_gain[i] * far_chain[k] for k in range(4) for i in range(3)]
    squares_of = [far_gain[i] * far_gain[m] for i, m in PAIRS]
    lists += squares_of + [q * far_reach[n] for n in range(3) for q in squares_of]
    block = over_senders(lists)

    def squares(power, i, m):
        at = 12 + power * 6 + PAIRS.index((min(i, m), max(i, m)))
        return block[at : at + 1, :]

    found = solve(lambda k, i: block[3 * k + i : 3 * k + i + 1, :], squares, [], 4)
    for k in range(4):
        z = sum(far_gain[i] * found[k][i] for i in range(3))
        for s in range(ST):
            b_out[s, k : k + 1, :] = z[s : s + 1, :]
    start(3, lambda b: b_out.at[b // 8], b_in, -1)


    atom_bond = inverse[0:16, :].astype(I32)
    bond_at = jnp.maximum(atom_bond - 1, 0)
    atom_label = lookup([label[t : t + 1, :] for t in range(BT)], bond_at // LANES, bond_at % LANES)
    row16 = lax.broadcasted_iota(I32, (16, LANES), 0)
    atom_label = jnp.where(
        jnp.logical_and(atom_bond > 0, row16 < AT), atom_label, 0.0
    ).astype(I32)
    label = label.astype(I32)

    def labelled(tiles, which):
        at = jnp.maximum(which - 1, 0)
        return jnp.where(which > 0, lookup(tiles, at // LANES, at % LANES), 0.0)

    unit = jnp.where(is_halo, 1.0, 0.0)
    chain, reach = [right], [unit]
    for _ in range(4):
        nxt = couple([chain[-1], reach[-1]])
        chain.append(nxt[0])
        reach.append(nxt[1])
    base = chain[0] + chain[1] + chain[2] + chain[3] + chain[4]
    grown = [reach[0]]
    for m in range(1, 5):
        grown.append(grown[-1] + reach[m])
    to_atoms([v * g for v in [base] + grown[:4] for g in gain])
    moves = []
    for n in range(15):
        moves.append(difference(n))
    all_of(3, b_in).wait_recv()
    back = merge(b_in, 4)

    def kind_rows(tiles, k):
        return [tiles[s][k : k + 1, :] for s in range(ST)]

    z = [labelled(kind_rows(back, k), label) for k in range(4)]
    sol_one = base
    for j in range(4):
        sol_one = sol_one + z[j] * grown[3 - j]
    current = None
    moved = []
    for i in range(3):
        ahead = head_new[i] - jnp.where(is_halo, 0.0, tail_new[i])
        step = moves[i]
        for j in range(4):
            step = step + z[j] * moves[3 * (1 + 3 - j) + i]
        stretch = ahead - step
        moved.append(stretch)
        current = stretch * stretch if current is None else current + stretch * stretch

    def second_right(scale, length, current):
        target = jnp.sqrt(jnp.maximum(2.0 * length * length - current, 0.5 * length * length))
        return scale * (length - target)

    chain_two = [jnp.where(is_halo, 0.0, second_right(scale, length, current))]
    tree_sums = times_ones(
        [reach[k] * chain_two[0] for k in range(1, 5)] + [unit * m for m in moved],
        trees_of[...],
    )
    for s in range(ST):
        c_out[s] = tree_sums[0:8, s * LANES : (s + 1) * LANES]
    start(4, lambda b: c_out.at[b // 8], c_in, 1)
    for _ in range(4):
        chain_two.append(couple([chain_two[-1]])[0])

    for n in range(15):
        for j in range(AT):
            gathered[n, j : j + 1, :] = sums[j, n : n + 1, :]
        gathered[n, AT:16, :] = jnp.zeros((16 - AT, LANES), F32)
    base_two = chain_two[0] + chain_two[1] + chain_two[2] + chain_two[3] + chain_two[4]
    to_atoms([v * g for v in (base_two, grown[4]) for g in gain])
    mass_atoms = jnp.concatenate(
        [table[j, 6:7, :] for j in range(AT)] + [jnp.zeros((16 - AT, LANES), F32)], axis=0
    )
    still = []
    for i in range(3):
        spread_base = jnp.concatenate(
            [gathered[i, j : j + 1, :] + sums[j, i : i + 1, :] for j in range(AT)]
            + [jnp.zeros((16 - AT, LANES), F32)],
            axis=0,
        )
        start_pos = jnp.concatenate(
            [table[j, i : i + 1, :] + table[j, 3 + i : 4 + i, :] for j in range(AT)]
            + [jnp.zeros((16 - AT, LANES), F32)],
            axis=0,
        )
        still.append(start_pos - mass_atoms * spread_base)
    trees = [[mass_atoms * gathered[3 * (1 + n) + i] for i in range(3)] for n in range(4)]
    no_atoms = jnp.zeros((16 - AT, LANES), F32)
    trees.append(
        [
            mass_atoms
            * jnp.concatenate([sums[j, 3 + i : 4 + i, :] for j in range(AT)] + [no_atoms], axis=0)
            for i in range(3)
        ]
    )
    all_of(2, a2_in).wait_recv()
    late = by_kind(merge(a2_in, 4), 3)
    feed.append(sum(pull[i] * late[i] for i in range(3)))
    next_chain()
    far_reach.append(
        far_own * far_reach[2] + turn[0] * far_reach[1] + turn[1] * far_own + turn[2]
    )
    last_sum = over_senders([far_gain[i] * far_chain[4] for i in range(3)])
    solve(lambda k, i: last_sum[i : i + 1, :], squares, found, 5)
    sent_total = [
        found[0][i] + found[1][i] + found[2][i] + found[3][i] + found[4][i] for i in range(3)
    ]
    sent_moved = [mine[i : i + 1, :] + mine[3 + i : 4 + i, :] - sent_total[i] for i in range(3)]
    number16 = row16 * LANES + lax.broadcasted_iota(I32, (16, LANES), 1)
    which = jnp.zeros((16, LANES), I32)
    for e in range(SEND):
        which = jnp.where(number16 == sent8[0:1, e : e + 1], e + 1, which)

    all_of(4, c_in).wait_recv()
    far_two = by_kind(merge(c_in, 8), 7)
    apart = [far_two[4 + i] - sent_moved[i] for i in range(3)]
    far_right_two = second_right(
        far_scale, far_length, apart[0] * apart[0] + apart[1] * apart[1] + apart[2] * apart[2]
    )
    far_right_two = jnp.where(used, far_right_two, 0.0)
    far_chain_two = [far_right_two]
    for k in range(4):
        far_chain_two.append(far_two[k] + far_reach[k] * far_right_two)
    block_two = over_senders([far_gain[i] * far_chain_two[k] for k in range(5) for i in range(3)])
    found_two = solve(lambda k, i: block_two[3 * k + i : 3 * k + i + 1, :], squares, [], 5)
    for k in range(4):
        z_two = sum(far_gain[i] * found_two[k][i] for i in range(3))
        for s in range(ST):
            d_out[s, k : k + 1, :] = z_two[s : s + 1, :]
    for s in range(ST):
        d_out[s, 4:5, :] = far_right_two[s : s + 1, :]
        d_out[s, 5:8, :] = jnp.zeros((3, LANES), F32)
    start(5, lambda b: d_out.at[b // 8], d_in, -1)

    for i in range(3):
        total = sent_total[i]
        for k in range(5):
            total = total + found_two[k][i]
        own_move = take(jnp.broadcast_to(total, (16, LANES)), jnp.maximum(which - 1, 0))
        still[i] = still[i] - jnp.where(which > 0, own_move, 0.0)

    all_of(5, d_in).wait_recv()
    last = merge(d_in, 8)
    result = sol_one + base_two
    for j in range(5):
        result = result + labelled(kind_rows(last, j), label) * grown[3 - j if j < 4 else 4]
    for t in range(BT):
        mult_ref[:, t * LANES : (t + 1) * LANES] = result[t : t + 1, :]
    both = [[back[s][k : k + 1, :] + last[s][k : k + 1, :] for s in range(ST)] for k in range(4)]
    both.append(kind_rows(last, 4))
    for j in range(5):
        z_atom = labelled(both[j], atom_label)
        for i in range(3):
            still[i] = still[i] - z_atom * trees[3 - j if j < 4 else 4][i]
    for i in range(3):
        for j in range(AT):
            at = i * ATOMS + j * LANES
            new_ref[:, at : at + LANES] = still[i][j : j + 1, :]

    for stage, target in ((0, r0_in), (1, a_in), (2, a2_in), (3, b_in), (4, c_in), (5, d_in)):
        all_of(stage, target).wait_send()


def write_out(new_ref, mult_ref, new_out, mult_out):
    new_out[...] = new_ref[...]
    mult_out[...] = mult_ref[...]


def solution(mesh):
    sizes = tuple(mesh.shape[n] for n in ("gx", "gy", "gz"))

    def per_device(old_pos, displacement, inv_mass, bond_head, bond_tail, send_list):
        near = len(BLOCKS)
        vmem = pl.BlockSpec(memory_space=pltpu.VMEM)
        new_pos, multipliers = pl.pallas_call(
            functools.partial(kernel, sizes),
            out_shape=(pltpu.VMEM((1, 3 * ATOMS), F32), pltpu.VMEM((1, BONDS), F32)),
            in_specs=[pl.BlockSpec(memory_space=pl.ANY)] * 6,
            out_specs=(vmem, vmem),
            scratch_shapes=[
                pltpu.VMEM((3, 1, ATOMS), F32),
                pltpu.VMEM((3, 1, ATOMS), F32),
                pltpu.VMEM((1, ATOMS), F32),
                pltpu.VMEM((1, BONDS), I32),
                pltpu.VMEM((1, BONDS), I32),
                pltpu.VMEM((1, SEND), I32),
                pltpu.SemaphoreType.DMA((6,)),
                pltpu.VMEM((AT, 8, LANES), F32),
                pltpu.VMEM((2, 8, LANES), I32),
                pltpu.VMEM((8, BONDS, LANES), F32),
                pltpu.VMEM((BONDS, ATOMS), jnp.bfloat16),
                pltpu.VMEM((BONDS, ST * LANES), jnp.bfloat16),
                pltpu.VMEM((BONDS, BONDS), F32),
                pltpu.VMEM((AT + ST, 8, LANES), F32),
                pltpu.VMEM((AT + ST, LANES), F32),
                pltpu.VMEM((2, 8, LANES), F32),
                pltpu.VMEM((2, 8, LANES), F32),
                pltpu.VMEM((2, BT, 32, LANES), F32),
                pltpu.VMEM((BONDS, 32), jnp.bfloat16),
                pltpu.VMEM((AT, 16, LANES), F32),
                pltpu.VMEM((8, 40, LANES), F32),
                pltpu.VMEM((15, 16, LANES), F32),
                pltpu.VMEM((8, LANES), F32),
                pltpu.VMEM((near, 8, LANES), F32),
                pltpu.VMEM((ST, 4, LANES), F32),
                pltpu.VMEM((ST, 4, LANES), F32),
                pltpu.VMEM((ST, 8, LANES), F32),
                pltpu.VMEM((ST, 8, LANES), F32),
                pltpu.VMEM((near, 8, LANES), F32),
                pltpu.VMEM((near, 8, LANES), F32),
                pltpu.VMEM((near, 4, LANES), F32),
                pltpu.VMEM((near, 4, LANES), F32),
                pltpu.VMEM((near, 8, LANES), F32),
                pltpu.VMEM((near, 8, LANES), F32),
                pltpu.SemaphoreType.DMA((6,)),
                pltpu.SemaphoreType.DMA((6,)),
            ],
            compiler_params=pltpu.CompilerParams(collective_id=0, has_side_effects=True),
        )(
            old_pos.reshape(3, 1, ATOMS),
            displacement.reshape(3, 1, ATOMS),
            inv_mass.reshape(1, ATOMS),
            bond_head.reshape(1, BONDS),
            bond_tail.reshape(1, BONDS),
            send_list.reshape(1, SEND),
        )
        new_pos, multipliers = pl.pallas_call(
            write_out,
            out_shape=(
                jax.ShapeDtypeStruct((1, 3 * ATOMS), F32),
                jax.ShapeDtypeStruct((1, BONDS), F32),
            ),
            in_specs=[vmem] * 2,
            out_specs=(vmem, vmem),
        )(
            pltpu.with_memory_space_constraint(new_pos, pltpu.VMEM),
            pltpu.with_memory_space_constraint(multipliers, pltpu.VMEM),
        )
        return new_pos.reshape(old_pos.shape), multipliers.reshape(bond_head.shape)

    return jax.shard_map(
        per_device,
        mesh=mesh,
        in_specs=(
            P(None, "gx", "gy", "gz", None),
            P(None, "gx", "gy", "gz", None),
            P("gx", "gy", "gz", None),
            P("gx", "gy", "gz", None),
            P("gx", "gy", "gz", None),
            P("gx", "gy", "gz", None),
        ),
        out_specs=(P(None, "gx", "gy", "gz", None), P("gx", "gy", "gz", None)),
        check_vma=False,
    )
```
